128 devices in a mesh: seq: 16 (over y, x), batch: 8 (over z, core).
Axes of the slice: x: 4, y: 4, z: 4, core: 2. Of those that a mesh axis runs over, the one named last changes fastest.
Arguments:
- queries: bfloat16 [16384, 4096], P(('batch', 'seq')), parts along dimension 0, may hold values from -6 to 6
- key_vectors: bfloat16 [16384, 4096], P(('batch', 'seq')), parts along dimension 0, may hold values from -6 to 6
- value_vectors: bfloat16 [16384, 4096], P(('batch', 'seq')), parts along dimension 0, may hold values from -6 to 6
- residual_in: bfloat16 [16384, 4096], P(('batch', 'seq')), parts along dimension 0, may hold values from -6 to 6
- input_logit: float32 [8, 16384], P(None, ('batch', 'seq')), parts along dimension 1, may hold values from -8 to 300
- forget_logit: float32 [8, 16384], P(None, ('batch', 'seq')), parts along dimension 1, may hold values from -3 to 13
- mix_gain: float32 [4096], replicated, may hold values from 0.1 to 1.9
- ffn_gain: float32 [4096], replicated, may hold values from 0.1 to 1.9
- expert_gate: bfloat16 [16, 4096, 704], P('seq'), may hold values from -0.09375 to 0.09375
- expert_up: bfloat16 [16, 4096, 704], P('seq'), may hold values from -0.09375 to 0.09375
- expert_down: bfloat16 [16, 704, 4096], P('seq'), may hold values from -0.21875 to 0.21875
- routes: int32 [16384, 2], P(('batch', 'seq')), parts along dimension 0, may hold values from 0 to 15, all different within a row; in each aligned block of 128 rows (0 to 127, 128 to 255, ...) at most 32 rows name the same one
- route_weight: float32 [16384, 2], P(('batch', 'seq')), parts along dimension 0, may hold values from 0.2 to 1
Outputs:
- block_out: bfloat16 [16384, 4096], P(('batch', 'seq')), parts along dimension 0
The draws below stay inside these ranges and needn't reach their ends.
There are 8 independent parts, one for each index of `batch`. The reference program is written for one: setup_inputs(seed, part) draws one part's arguments, and reference() takes and returns one part's arrays. A program takes and returns all parts, laid end to end along the dimension named above; an argument that names none is the same for every part. Nothing has to cross between parts.
Inputs may be any that keep to these rules, and one draw needn't show every extreme that they name: `routes`: each row names two different experts. Within the rows of one device no expert is named by more than 32 rows, and in some device one expert is named by exactly 32 rows.
All inputs are finite; a program needn't handle non-finite values.
Results may differ from the reference program's by a relative error of at most 0.0081.
Values may be sent and summed in bfloat16 or wider, within the bound.
A program may use at most 128 MiB of HBM per device.

```python
import math
import jax
import jax.numpy as jnp
import numpy as np
from jax import lax

MIXER_HEADS = 8
DH = 512
D = 4096
FF = 704
TOK_DEV = 128
SEQUENCE_LENGTH = 2048
EXPERTS = 16
CAP = 32


def draw_forget_logit(key, part):
    random_child_keys = jax.random.split(jax.random.fold_in(key, 11), 6)
    chooser = jax.random.uniform(random_child_keys[0], (MIXER_HEADS, 1))
    quick_head = chooser < 0.5
    horizon = TOK_DEV * jax.random.uniform(random_child_keys[1], (MIXER_HEADS, 1), minval=0.15, maxval=0.25)
    slow_rate = jnp.log(1.0 / 0.7) / SEQUENCE_LENGTH * jnp.ones((MIXER_HEADS, 1), jnp.float32)
    base_rate = jnp.where(quick_head, 1.0 / horizon, slow_rate)
    blocks = SEQUENCE_LENGTH // TOK_DEV
    device_factor = jnp.exp(jax.random.uniform(random_child_keys[2], (MIXER_HEADS, blocks), minval=-0.7, maxval=0.7))
    device_factor = jnp.repeat(device_factor, TOK_DEV, axis=1)
    roughness = jax.random.uniform(random_child_keys[3], (MIXER_HEADS, SEQUENCE_LENGTH), minval=0.5, maxval=1.5)
    forget_decay_speed = base_rate * device_factor * roughness
    spike_locations = jax.random.randint(random_child_keys[4], (3,), 0, SEQUENCE_LENGTH)
    spike_present = jnp.any(jnp.arange(SEQUENCE_LENGTH)[None, :] == spike_locations[:, None], axis=0)[None, :]
    spike_frequency = jax.random.uniform(random_child_keys[5], (MIXER_HEADS, SEQUENCE_LENGTH), minval=0.22, maxval=0.69)
    forget_decay_speed = jnp.where(spike_present, spike_frequency, forget_decay_speed)
    return jnp.log(1.0 / jnp.expm1(forget_decay_speed)).astype(jnp.float32)


def draw_input_logit(key, part):
    random_child_keys = jax.random.split(jax.random.fold_in(key, 23), 5)
    drawn = jax.random.normal(random_child_keys[4], (MIXER_HEADS, SEQUENCE_LENGTH)) * 1.5 - 1.0
    return jnp.clip(drawn, -8.0, 8.0).astype(jnp.float32)


def block_levels(rng, dims, shards, least, largest):
    def one(dim, blocks):
        draws = jax.random.uniform(jax.random.fold_in(jax.random.fold_in(rng, 6), dim), (blocks,), jnp.float32, least / len(shards), largest / len(shards))
        return jnp.repeat(jnp.exp(draws), dims[dim] // blocks).reshape((-1,) + (1,) * (len(dims) - dim - 1))

    gain = one(*shards[0])
    for cut in shards[1:]:
        gain = gain * one(*cut)
    return gain


def shared_out(key, own, number, rows, number_of, top, reach, lean):
    sequence = jax.random.permutation(key, number_of)
    crowded, common = portions_of(number_of, rows * top, reach, lean, True), portions_of(number_of, rows * top, reach, lean, False)
    places = jnp.arange(number_of)

    def named(sizes, turn):
        used = int((sizes > 0).sum())
        fixed = max(1, used // 4)
        shifted = fixed + (places - fixed + turn * (used - fixed)) % max(1, number_of - fixed)
        return jnp.zeros((number_of,), jnp.int32).at[sequence[jnp.where(places < fixed, places, shifted)]].set(jnp.asarray(sizes, jnp.int32))

    sizes = jnp.where(number % 4 == 0, named(crowded, number // 4), named(common, number - number // 4 - 1))
    mixed = jax.random.permutation(jax.random.fold_in(own, 3), number_of)
    donor, receiver = mixed[0:number_of // 2 * 2:2], mixed[1:number_of // 2 * 2:2]
    slack = jnp.minimum(sizes[donor] - 1, reach - sizes[receiver]) // 2
    slack = jnp.where((donor == sequence[0]) | (receiver == sequence[0]) | (sizes[receiver] == 0), 0, jnp.maximum(slack, 0))
    shifted = jax.random.randint(jax.random.fold_in(own, 4), (number_of // 2,), 0, 1 << 20) % (slack + 1)
    sizes = sizes.at[donor].add(-shifted).at[receiver].add(shifted)
    members = jnp.searchsorted(jnp.cumsum(sizes), jnp.arange(rows * top), side="right").astype(jnp.int32)
    grid = members.reshape(top, rows).T
    grid = grid[jax.random.permutation(jax.random.fold_in(own, 1), rows)]
    turn = jax.random.randint(jax.random.fold_in(own, 2), (rows, 1), 0, top)
    return jnp.take_along_axis(grid, (jnp.arange(top)[None, :] + turn) % top, axis=1)


def portions_of(amount, total, limit, skew, full):
    weights = [(1 << 20) // math.isqrt(standing ** skew) + 1 for standing in range(1, amount + 1)]
    largest = limit if full else min(limit, max(-(-total // amount), total * weights[0] // sum(weights)))
    least = 1 if total - largest >= amount - 1 else 0
    given, surplus = [largest] + [least] * (amount - 1), total - largest - least * (amount - 1)
    while surplus > 0:
        free = [i for i in range(1, amount) if given[i] < largest] or [i for i in range(1, amount) if given[i] < limit]
        whole, remaining = sum([weights[i] for i in free]), surplus
        for i in free:
            more = min(limit - given[i], max(1, remaining * weights[i] // whole), surplus)
            given[i] = given[i] + more
            surplus = surplus - more
    return np.array(given)


def scatter_about(own_key, extent, spread, bound, cuts=(), kind=jnp.bfloat16):
    entries = spread * jax.random.normal(own_key, extent, jnp.float32)
    if cuts:
        entries = entries * block_levels(own_key, extent, cuts, -0.22, 0.18)
    return jnp.clip(entries, -bound, bound).astype(kind)


def setup_inputs(seed: int = 0, part: int = 0) -> dict:
    seeds = jax.random.split(jax.random.key(seed), 14)
    own_keys = jax.random.split(jax.random.fold_in(seeds[13], part), 14)
    queries = scatter_about(own_keys[0], (SEQUENCE_LENGTH, D), 1.0, 6.0, ((0, 16),))
    key_vectors = scatter_about(own_keys[1], (SEQUENCE_LENGTH, D), 1.0, 6.0, ((0, 16),))
    value_vectors = scatter_about(own_keys[2], (SEQUENCE_LENGTH, D), 1.0, 6.0, ((0, 16),))
    residual_in = scatter_about(own_keys[3], (SEQUENCE_LENGTH, D), 1.0, 6.0, ((0, 16),))
    input_logit = draw_input_logit(jax.random.fold_in(jax.random.fold_in(seeds[13], part), 71), part)
    forget_logit = draw_forget_logit(jax.random.fold_in(jax.random.fold_in(seeds[13], part), 71), part)
    mix_gain = jnp.clip(1.0 + 0.18 * jax.random.normal(seeds[6], (D,), jnp.float32), 0.1, 1.9)
    ffn_gain = jnp.clip(1.0 + 0.18 * jax.random.normal(seeds[7], (D,), jnp.float32), 0.1, 1.9)
    expert_gate = scatter_about(seeds[8], (EXPERTS, D, FF), D ** -0.5, 0.09375, ((0, 16),))
    expert_up = scatter_about(seeds[9], (EXPERTS, D, FF), D ** -0.5, 0.09375, ((0, 16),))
    expert_down = scatter_about(seeds[10], (EXPERTS, FF, D), FF ** -0.5, 0.21875, ((0, 16),))
    routes_keys = jax.random.split(jax.random.fold_in(own_keys[11], 1), SEQUENCE_LENGTH // TOK_DEV)
    routes_turns = jax.random.permutation(jax.random.fold_in(own_keys[11], 3), SEQUENCE_LENGTH // TOK_DEV)
    routes = jax.vmap(lambda own, number: shared_out(jax.random.fold_in(own_keys[11], 2), own, number, TOK_DEV, EXPERTS, 2, CAP, 2))(routes_keys, routes_turns).reshape((SEQUENCE_LENGTH, 2))
    route_weight = jnp.clip(0.2 + 0.8 * jax.random.uniform(own_keys[12], (SEQUENCE_LENGTH, 2), jnp.float32) ** block_levels(own_keys[12], (SEQUENCE_LENGTH, 2), ((0, 16),), -0.2, 0.2), 0.2, 1.0)
    return dict(queries=queries, key_vectors=key_vectors, value_vectors=value_vectors, residual_in=residual_in, input_logit=input_logit, forget_logit=forget_logit, mix_gain=mix_gain, ffn_gain=ffn_gain, expert_gate=expert_gate, expert_up=expert_up, expert_down=expert_down, routes=routes, route_weight=route_weight)


NEG_FILL = -1e+30
EPSILON = 1e-06

def join_states(earlier, later):
    total_early, state_early, normv_early, peak_early = earlier
    total_late, state_late, normv_late, peak_late = later
    carried = total_late + peak_early
    peak_new = jnp.maximum(carried, peak_late)
    scale_early = jnp.exp(carried - peak_new)
    scale_late = jnp.exp(peak_late - peak_new)
    state_new = scale_early[..., None] * state_early + scale_late[..., None] * state_late
    normv_new = scale_early * normv_early + scale_late * normv_late
    return (total_early + total_late, state_new, normv_new, peak_new)

def block_summary(keys_three, values_three, log_forget, input_gate):
    cumul_log = jnp.cumsum(log_forget, axis=1)
    tail_log = cumul_log[:, -1:] - cumul_log + input_gate
    peak_log = lax.optimization_barrier(jnp.max(tail_log, axis=1))
    weight = jnp.exp(tail_log - peak_log[:, None])
    weighted = keys_three.astype(jnp.float32) * jnp.transpose(weight)[:, :, None]
    rounded = lax.optimization_barrier(weighted.astype(jnp.bfloat16))
    state_mat = jnp.einsum('thd,the->hde', rounded.astype(jnp.float32), values_three.astype(jnp.float32))
    norm_vec = lax.optimization_barrier(jnp.sum(weighted, axis=0))
    total_log = jnp.broadcast_to(cumul_log[:, -1:], norm_vec.shape)
    peak_full = jnp.broadcast_to(peak_log[:, None], norm_vec.shape)
    return (total_log, state_mat, norm_vec, peak_full)

def block_output(queries_three, keys_three, values_three, log_forget, input_gate, carry_in):
    length_block = queries_three.shape[0]
    inverse_root = 1.0 / math.sqrt(queries_three.shape[2])
    cumul_log = jnp.cumsum(log_forget, axis=1)
    log_weight = cumul_log[:, :, None] - cumul_log[:, None, :] + input_gate[:, None, :]
    causal = jnp.arange(length_block)[:, None] >= jnp.arange(length_block)[None, :]
    log_weight = jnp.where(causal[None], log_weight, NEG_FILL)
    carry_total, carry_state, carry_norm, carry_peak = carry_in
    carried = cumul_log + carry_peak[:, 0:1]
    peak_log = jnp.maximum(lax.optimization_barrier(jnp.max(log_weight, axis=2)), carried)
    decay_mat = jnp.exp(log_weight - peak_log[:, :, None])
    query_float = queries_three.astype(jnp.float32)
    scores = jnp.einsum('thd,shd->hts', query_float, keys_three.astype(jnp.float32)) * inverse_root
    coef = decay_mat * scores
    denom_sum = lax.optimization_barrier(jnp.sum(coef, axis=2))
    coef_round = lax.optimization_barrier(coef.astype(jnp.bfloat16))
    numer_sum = jnp.einsum('hts,she->the', coef_round.astype(jnp.float32), values_three.astype(jnp.float32))
    carry_reach = jnp.exp(carried - peak_log) * inverse_root
    from_state = jnp.einsum('thd,hde->the', query_float, carry_state, precision=lax.Precision.HIGHEST)
    from_norm = jnp.einsum('thd,hd->ht', query_float, carry_norm, precision=lax.Precision.HIGHEST)
    numer_sum = numer_sum + jnp.transpose(carry_reach)[:, :, None] * from_state
    denom_sum = denom_sum + carry_reach * from_norm
    floor_sum = jnp.maximum(jnp.abs(denom_sum), 1.0)
    return numer_sum / jnp.transpose(floor_sum)[:, :, None]

def reference(queries, key_vectors, value_vectors, residual_in, input_logit, forget_logit, mix_gain, ffn_gain, expert_gate, expert_up, expert_down, routes, route_weight):
    log_forget = jax.nn.log_sigmoid(forget_logit)
    blocks = SEQUENCE_LENGTH // TOK_DEV

    def split_rows(array):
        return array.reshape(blocks, TOK_DEV, MIXER_HEADS, DH)

    def split_gates(array):
        return jnp.transpose(array.reshape(MIXER_HEADS, blocks, TOK_DEV), (1, 0, 2))
    initial = (jnp.zeros((MIXER_HEADS, DH), jnp.float32), jnp.zeros((MIXER_HEADS, DH, DH), jnp.float32), jnp.zeros((MIXER_HEADS, DH), jnp.float32), jnp.full((MIXER_HEADS, DH), NEG_FILL, jnp.float32))

    def advance(carry_in, pieces):
        query_block, key_block, value_block, forget_block, input_block = pieces
        result = block_output(query_block, key_block, value_block, forget_block, input_block, carry_in)
        carry_out = join_states(carry_in, block_summary(key_block, value_block, forget_block, input_block))
        return (carry_out, result)
    unused, mixer_out = lax.scan(advance, initial, (split_rows(queries), split_rows(key_vectors), split_rows(value_vectors), split_gates(log_forget), split_gates(input_logit)))
    mixer_out = mixer_out.reshape(SEQUENCE_LENGTH, D)
    mixer_square = lax.optimization_barrier(jnp.mean(mixer_out * mixer_out, axis=1, keepdims=True))
    updated = (residual_in.astype(jnp.float32) + mixer_out * lax.rsqrt(mixer_square + EPSILON) * mix_gain).astype(jnp.bfloat16)
    updated_float = updated.astype(jnp.float32)
    updated_square = lax.optimization_barrier(jnp.mean(updated_float * updated_float, axis=1, keepdims=True))
    normed = (updated_float * lax.rsqrt(updated_square + EPSILON) * ffn_gain).astype(jnp.bfloat16)
    flat_routes = routes.reshape(blocks, 2 * TOK_DEV)
    matches = (flat_routes[:, :, None] == jnp.arange(EXPERTS, dtype=jnp.int32)[None, None, :]).astype(jnp.int32)
    before = jnp.cumsum(matches, axis=1) - matches
    position = lax.optimization_barrier(jnp.sum(before * matches, axis=2))
    source_index = jnp.arange(blocks, dtype=jnp.int32)[:, None]
    slot_index = (flat_routes * (blocks * CAP) + source_index * CAP + position).reshape(SEQUENCE_LENGTH, 2).astype(jnp.int32)
    buffer_rows = jnp.zeros((EXPERTS * blocks * CAP, D), jnp.bfloat16)
    buffer_rows = buffer_rows.at[slot_index[:, 0]].set(normed).at[slot_index[:, 1]].set(normed)

    def run_expert(pieces):
        row_block, gate_weight, up_weight, down_weight = pieces
        gate_val = jnp.dot(row_block, gate_weight, preferred_element_type=jnp.float32)
        up_val = jnp.dot(row_block, up_weight, preferred_element_type=jnp.float32)
        hidden = (jax.nn.silu(gate_val) * up_val).astype(jnp.bfloat16)
        return jnp.dot(hidden, down_weight, preferred_element_type=jnp.float32).astype(jnp.bfloat16)
    outputs = lax.map(run_expert, (buffer_rows.reshape(EXPERTS, blocks * CAP, D), expert_gate, expert_up, expert_down)).reshape(EXPERTS * blocks * CAP, D)
    first_out = outputs[slot_index[:, 0]].astype(jnp.float32)
    second_out = outputs[slot_index[:, 1]].astype(jnp.float32)
    expert_mix = route_weight[:, 0:1] * first_out + route_weight[:, 1:2] * second_out
    return (updated_float + expert_mix).astype(jnp.bfloat16)
```

```python
import functools
import math

import jax
import jax.numpy as jnp
from jax import lax
from jax.experimental import pallas as pl
from jax.experimental.pallas import tpu as pltpu
from jax.sharding import PartitionSpec as P

NEG_FILL = -1e30
EPSILON = 1e-06
MESH = pl.DeviceIdType.MESH
HEADS = 8
DH = 512
D = 4096
FF = 704
TOK = 128
CAP = 32
DEV = 16
CHUNK = 256
ROOT = 1.0 / math.sqrt(DH)
ORDER = (0, 1, 3, 4, 12, 2, 8, 10, 5, 15, 7, 13, 6, 14, 9, 11)
NEAR = ((0, 1), (0, 3), (1, 0), (1, 1), (1, 3), (0, 2), (1, 2))


def peer_of(me, offset):
    row = lax.rem(me // 4 + offset // 4, 4)
    col = lax.rem(lax.rem(me, 4) + offset % 4, 4)
    return row * 4 + col


def entry_barrier(me):
    barrier = pltpu.get_barrier_semaphore()
    for offset in range(1, DEV):
        pl.semaphore_signal(
            barrier, inc=1, device_id={"seq": peer_of(me, offset)}, device_id_type=MESH
        )
    pl.semaphore_wait(barrier, DEV - 1)


def remote(src, dst, send, recv, device):
    return pltpu.make_async_remote_copy(
        src_ref=src,
        dst_ref=dst,
        send_sem=send,
        recv_sem=recv,
        device_id={"seq": device},
        device_id_type=MESH,
    )


def scan_lanes(x, op, fill):
    lane = lax.broadcasted_iota(jnp.int32, x.shape, 1)
    step = 1
    while step < x.shape[1]:
        x = op(x, jnp.where(lane >= step, pltpu.roll(x, step, 1), fill))
        step *= 2
    return x


def three_parts(x):
    high = x.astype(jnp.bfloat16).astype(jnp.float32)
    rest = x - high
    middle = rest.astype(jnp.bfloat16).astype(jnp.float32)
    return high, middle, rest - middle


def nt_dot(a, b):
    return lax.dot_general(a, b, (((1,), (1,)), ((), ())), preferred_element_type=jnp.float32)


def mixer_kernel(
    q_in, k_in, v_in, gate_i, gate_f, mix,
    qb, kb, vb, gbi, gbf, chi, clo, sacc, zst, z_in, st_in, st_out, z_out, ob, rowi, rowf, grow, tcol,
    own_sem, gs, gr, ks, kr, vs, vr, qs, qr, os, orr, ss, sr,
):
    me = lax.axis_index("seq")
    half = me // 8
    base = half * 8
    local = me - base
    head = lax.rem(local + 4 * half, 8)

    def rows(j):
        return pl.ds(pl.multiple_of(j * TOK, TOK), TOK)

    def head_columns(h):
        return pl.ds(pl.multiple_of(h * DH, DH), DH)

    own = [
        pltpu.make_async_copy(src.at[:, head_columns(head)], dst.at[rows(local), :], own_sem.at[n])
        for n, (src, dst) in enumerate(((k_in, kb), (v_in, vb), (q_in, qb)))
    ]
    for copy in own:
        copy.start()
    entry_barrier(me)

    sent = []
    for offset in range(1, DEV):
        to = peer_of(me, offset)
        for src, dst, n in ((gate_i, gbi, 0), (gate_f, gbf, 1)):
            copy = remote(src, dst.at[me], gs.at[n, offset], gr.at[n, me], to)
            copy.start()
            sent.append(copy)
    gbi[me] = gate_i[...]
    gbf[me] = gate_f[...]

    def send_all(src, dst, send, recv):
        for n, (dy, dx) in enumerate(NEAR):
            to = lax.rem(local // 4 + dy, 2) * 4 + lax.rem(lax.rem(local, 4) + dx, 4)
            to_head = lax.rem(to + 4 * half, 8)
            copy = remote(
                src.at[:, head_columns(to_head)], dst.at[rows(local), :], send.at[n], recv.at[local], base + to
            )
            copy.start()
            sent.append(copy)

    send_all(k_in, kb, ks, kr)
    send_all(v_in, vb, vs, vr)
    send_all(q_in, qb, qs, qr)

    for offset in range(1, DEV):
        src = peer_of(me, offset)
        remote(gate_i, gbi.at[src], gs.at[0, offset], gr.at[0, src], me).wait_recv()
        remote(gate_f, gbf.at[src], gs.at[1, offset], gr.at[1, src], me).wait_recv()
    for b in range(DEV):
        rowi[b // 2 : b // 2 + 1, (b % 2) * TOK : (b % 2 + 1) * TOK] = gbi[b, pl.ds(head, 1), :]
        rowf[b // 2 : b // 2 + 1, (b % 2) * TOK : (b % 2 + 1) * TOK] = gbf[b, pl.ds(head, 1), :]
    x = rowf[...]
    log_forget = jnp.minimum(x, 0.0) - jnp.log1p(jnp.exp(-jnp.abs(x)))
    cumul = scan_lanes(log_forget, jnp.add, 0.0)
    lift = rowi[...] - cumul
    lift_max = scan_lanes(lift, jnp.maximum, NEG_FILL)
    decay = cumul[:, CHUNK - 1 : CHUNK]
    peak_in = decay + lift_max[:, CHUNK - 1 : CHUNK]
    peaks = [jnp.full((1, 1), NEG_FILL, jnp.float32)]
    for c in range(8):
        peaks.append(jnp.maximum(decay[c : c + 1] + peaks[-1], peak_in[c : c + 1]))
    first = half == 0
    scales = []
    since = jnp.ones((1, 1), jnp.float32)
    row8 = lax.broadcasted_iota(jnp.int32, (8, CHUNK), 0)
    for c in range(4):
        before = jnp.where(first, peaks[c], peaks[4 + c])
        after = jnp.where(first, peaks[c + 1], peaks[5 + c])
        dec = jnp.where(first, decay[c : c + 1], decay[4 + c : 5 + c])
        lift_c = jnp.where(first, lift[c : c + 1], lift[4 + c : 5 + c])
        top = jnp.maximum(jnp.where(first, lift_max[c : c + 1], lift_max[4 + c : 5 + c]), before)
        weight = jnp.exp(dec + lift_c - after)
        reach = jnp.exp(before - top) * ROOT
        packed = jnp.where(
            row8 == 0, weight, jnp.where(row8 == 1, top, jnp.where(row8 == 2, reach, reach * since))
        )
        tcol[c] = jnp.transpose(packed)
        grow[c] = lift_c
        scales.append(jnp.exp(dec + before - after))
        since = since * scales[-1]

    for c in range(4):
        for j in (2 * c, 2 * c + 1):

            @pl.when(j != local)
            def _():
                remote(kb.at[rows(j), :], kb.at[rows(j), :], ks.at[0], kr.at[j], me).wait_recv()
                remote(vb.at[rows(j), :], vb.at[rows(j), :], vs.at[0], vr.at[j], me).wait_recv()

            @pl.when(j == local)
            def _():
                own[0].wait()
                own[1].wait()

        weighted = kb[c * CHUNK : (c + 1) * CHUNK, :].astype(jnp.float32) * tcol[c][:, 0:1]
        fresh = lax.dot_general(
            weighted.astype(jnp.bfloat16),
            vb[c * CHUNK : (c + 1) * CHUNK, :],
            (((0,), (0,)), ((), ())),
            preferred_element_type=jnp.float32,
        )
        fresh_z = jnp.sum(weighted, axis=0, keepdims=True)
        if c == 0:
            chi[0] = jnp.zeros((DH, DH), jnp.bfloat16)
            clo[0] = jnp.zeros((DH, DH), jnp.bfloat16)
            zst[0] = jnp.zeros((1, DH), jnp.float32)
            z_now = fresh_z
            state = fresh
        else:
            state = scales[c] * sacc[...] + fresh
            z_now = scales[c] * z_now + fresh_z
        high = state.astype(jnp.bfloat16)
        if c < 3:
            sacc[...] = state
            zst[c + 1] = z_now
            chi[c + 1] = high
            clo[c + 1] = (state - high.astype(jnp.float32)).astype(jnp.bfloat16)
        else:
            st_out[...] = high
            z_out[...] = jnp.broadcast_to(z_now, (8, DH))

    next_device = 8 + lax.rem(local + 4, 8)
    state_copy = remote(st_out, st_in, ss.at[0], sr.at[0], next_device)
    z_copy = remote(z_out, z_in, ss.at[1], sr.at[1], next_device)

    @pl.when(half == 0)
    def _():
        state_copy.start()
        z_copy.start()
        z_in[...] = jnp.zeros((8, DH), jnp.float32)

    @pl.when(half == 1)
    def _():
        state_copy.wait_recv()
        z_copy.wait_recv()

    causal = lax.broadcasted_iota(jnp.int32, (CHUNK, CHUNK), 0) >= lax.broadcasted_iota(
        jnp.int32, (CHUNK, CHUNK), 1
    )
    z_row = lax.broadcasted_iota(jnp.int32, (8, DH), 0)

    @pl.loop(0, 4)
    def _(i):
        c = lax.rem(i + 1 + local // 2, 4)
        for jj in range(2):
            j = 2 * c + jj

            @pl.when(j != local)
            def _():
                remote(qb.at[rows(j), :], qb.at[rows(j), :], qs.at[0], qr.at[j], me).wait_recv()

            @pl.when(j == local)
            def _():
                own[2].wait()

        part = pl.ds(pl.multiple_of(c * CHUNK, CHUNK), CHUNK)
        query = qb[part, :]
        value = vb[part, :]
        columns = tcol[c]
        top, reach, reach0 = columns[:, 1:2], columns[:, 2:3], columns[:, 3:4]
        weight = jnp.exp(jnp.where(causal, grow[c] - top, NEG_FILL))
        coef = weight * (nt_dot(query, kb[part, :]) * ROOT)
        denom = jnp.sum(coef, axis=1, keepdims=True)
        numer = jnp.dot(coef.astype(jnp.bfloat16), value, preferred_element_type=jnp.float32)
        held = jnp.dot(query, chi[c], preferred_element_type=jnp.float32)
        held += jnp.dot(query, clo[c], preferred_element_type=jnp.float32)
        parts = three_parts(zst[c]) + three_parts(z_in[0:1, :])
        z_all = jnp.zeros((8, DH), jnp.float32)
        for n, piece in enumerate(parts):
            z_all = jnp.where(z_row == n, piece, z_all)
        norm = nt_dot(query, z_all.astype(jnp.bfloat16))
        denom += reach * (norm[:, 0:1] + norm[:, 1:2] + norm[:, 2:3])
        denom += reach0 * (norm[:, 3:4] + norm[:, 4:5] + norm[:, 5:6])
        numer += reach * held

        def finish(total):
            ob[part, :] = (total / jnp.maximum(jnp.abs(denom), 1.0)).astype(jnp.bfloat16)

        @pl.when(half == 0)
        def _():
            finish(numer)

        @pl.when(half == 1)
        def _():
            finish(numer + reach0 * jnp.dot(query, st_in[...], preferred_element_type=jnp.float32))

        for jj in range(2):
            j = 2 * c + jj

            @pl.when(j != local)
            def _():
                remote(ob.at[rows(j), :], mix.at[head], os.at[j], orr.at[head], base + j).start()

            @pl.when(j == local)
            def _():
                mix[head] = ob[rows(j), :]

    for copy in sent:
        copy.wait_send()

    @pl.when(half == 0)
    def _():
        state_copy.wait_send()
        z_copy.wait_send()

    for j in range(8):

        @pl.when(j != local)
        def _():
            from_head = lax.rem(j + 4 * half, 8)
            copy = remote(ob.at[rows(j), :], mix.at[from_head], os.at[j], orr.at[from_head], me)
            copy.wait_send()
            copy.wait_recv()


def expert_kernel(
    mix, residual, mix_gain, ffn_gain, routes, route_weight, w_gate, w_up, w_down, out,
    gate_v, up_v, down_v, disp, inbox, result, back, upd, normed, wmat, acc,
    w_sem, ds, dr, bs, br,
):
    me = lax.axis_index("seq")
    weights = [
        pltpu.make_async_copy(src, dst, w_sem.at[n])
        for n, (src, dst) in enumerate(((w_gate, gate_v), (w_up, up_v), (w_down, down_v)))
    ]
    for copy in weights:
        copy.start()
    entry_barrier(me)

    owner = jnp.zeros((DEV, TOK), jnp.int32)
    row16 = lax.broadcasted_iota(jnp.int32, (DEV, TOK), 0)
    for n, offset in enumerate(ORDER):
        owner = jnp.where(row16 == n, peer_of(me, offset), owner)
    hit0 = routes[0:1, :] == owner
    hit1 = routes[1:2, :] == owner
    match = jnp.where(hit0 | hit1, 1.0, 0.0).astype(jnp.bfloat16)
    earlier = lax.broadcasted_iota(jnp.int32, (TOK, TOK), 0) < lax.broadcasted_iota(
        jnp.int32, (TOK, TOK), 1
    )
    position = jnp.dot(
        match, jnp.where(earlier, 1.0, 0.0).astype(jnp.bfloat16), preferred_element_type=jnp.float32
    )
    slot = position + (row16 * CAP).astype(jnp.float32)
    slot0 = jnp.sum(jnp.where(hit0, slot, 0.0), axis=0, keepdims=True)
    slot1 = jnp.sum(jnp.where(hit1, slot, 0.0), axis=0, keepdims=True)
    row8 = lax.broadcasted_iota(jnp.int32, (8, TOK), 0)
    packed = jnp.where(
        row8 == 0,
        slot0,
        jnp.where(row8 == 1, slot1, jnp.where(row8 == 2, route_weight[0:1, :], route_weight[1:2, :])),
    )
    columns = jnp.transpose(packed)
    lane = lax.broadcasted_iota(jnp.int32, (TOK, DEV * CAP), 1).astype(jnp.float32)
    share = jnp.where(lane == columns[:, 0:1], columns[:, 2:3], 0.0) + jnp.where(
        lane == columns[:, 1:2], columns[:, 3:4], 0.0
    )
    high = share.astype(jnp.bfloat16)
    low = (share - high.astype(jnp.float32)).astype(jnp.bfloat16)
    for g in range(4):
        wmat[g, 0:TOK, :] = high[:, g * TOK : (g + 1) * TOK]
        wmat[g, TOK : 2 * TOK, :] = low[:, g * TOK : (g + 1) * TOK]

    square = jnp.zeros((TOK, 1), jnp.float32)
    for h in range(HEADS):
        part = mix[h].astype(jnp.float32)
        square += jnp.sum(part * part, axis=1, keepdims=True)
    scale = lax.rsqrt(square * (1.0 / D) + EPSILON)
    square = jnp.zeros((TOK, 1), jnp.float32)
    for h in range(HEADS):
        cols = slice(h * DH, (h + 1) * DH)
        part = residual[:, cols].astype(jnp.float32) + mix[h].astype(jnp.float32) * scale * mix_gain[:, cols]
        rounded = part.astype(jnp.bfloat16)
        upd[:, cols] = rounded
        part = rounded.astype(jnp.float32)
        square += jnp.sum(part * part, axis=1, keepdims=True)
    scale = lax.rsqrt(square * (1.0 / D) + EPSILON)
    for h in range(HEADS):
        cols = slice(h * DH, (h + 1) * DH)
        part = upd[:, cols].astype(jnp.float32)
        acc[:, cols] = part
        normed[:, cols] = (part * scale * ffn_gain[:, cols]).astype(jnp.bfloat16)

    pieces = 4
    depth = CAP // pieces
    for g in range(4):
        target = lax.broadcasted_iota(jnp.int32, (TOK, TOK), 0) + g * TOK
        pick = jnp.where((target == slot0.astype(jnp.int32)) | (target == slot1.astype(jnp.int32)), 1.0, 0.0)
        pick = pick.astype(jnp.bfloat16)
        for h in range(HEADS):
            cols = slice(h * DH, (h + 1) * DH)
            rows = jnp.dot(pick, normed[:, cols], preferred_element_type=jnp.float32)
            disp[g * TOK : (g + 1) * TOK, cols] = rows.astype(jnp.bfloat16)
        for p in range(pieces):
            for n in range(4 * g, 4 * g + 4):
                if n == 0:
                    continue
                piece = pl.ds(n * CAP + p * depth, depth)
                remote(
                    disp.at[piece, :], inbox.at[piece, :], ds.at[n], dr.at[n], peer_of(me, ORDER[n])
                ).start()
    inbox[0:CAP, :] = disp[0:CAP, :]

    def slot_rows(n):
        return pl.ds(n * CAP, CAP)

    for copy in weights:
        copy.wait()

    for g in range(4):
        for n in range(4 * g, 4 * g + 4):
            if n > 0:
                remote(disp.at[slot_rows(n), :], inbox.at[slot_rows(n), :], ds.at[n], dr.at[n], me).wait_recv()
        if g == 0:
            pass
        rows = inbox[g * TOK : (g + 1) * TOK, :]
        gate = nt_dot(rows, gate_v[...])
        up = nt_dot(rows, up_v[...])
        hidden = (gate / (1.0 + jnp.exp(-gate)) * up).astype(jnp.bfloat16)
        for h in range(HEADS):
            cols = slice(h * DH, (h + 1) * DH)
            result[g * TOK : (g + 1) * TOK, cols] = jnp.dot(
                hidden, down_v[:, cols], preferred_element_type=jnp.float32
            ).astype(jnp.bfloat16)
        for p in range(pieces):
            for n in range(4 * g, 4 * g + 4):
                if n == 0:
                    continue
                piece = pl.ds(n * CAP + p * depth, depth)
                back_to = peer_of(me, (4 - ORDER[n] // 4) % 4 * 4 + (4 - ORDER[n] % 4) % 4)
                remote(result.at[piece, :], back.at[piece, :], bs.at[n], br.at[n], back_to).start()
    back[0:CAP, :] = result[0:CAP, :]

    for g in range(4):
        for n in range(4 * g, 4 * g + 4):
            if n > 0:
                remote(result.at[slot_rows(n), :], back.at[slot_rows(n), :], bs.at[n], br.at[n], me).wait_recv()
        for h in range(HEADS):
            cols = slice(h * DH, (h + 1) * DH)
            both = jnp.dot(wmat[g], back[g * TOK : (g + 1) * TOK, cols], preferred_element_type=jnp.float32)
            total = acc[:, cols] + both[0:TOK, :] + both[TOK : 2 * TOK, :]
            if g < 3:
                acc[:, cols] = total
            else:
                out[:, cols] = total.astype(jnp.bfloat16)
    for n in range(1, DEV):
        remote(disp.at[slot_rows(n), :], inbox.at[slot_rows(n), :], ds.at[n], dr.at[n], me).wait_send()
        remote(result.at[slot_rows(n), :], back.at[slot_rows(n), :], bs.at[n], br.at[n], me).wait_send()


def shards(
    queries, key_vectors, value_vectors, residual_in, input_logit, forget_logit, mix_gain, ffn_gain,
    expert_gate, expert_up, expert_down, routes, route_weight,
):
    vmem = pl.BlockSpec(memory_space=pltpu.VMEM)
    hbm = pl.BlockSpec(memory_space=pl.ANY)
    dma = pltpu.SemaphoreType.DMA
    bf16, f32 = jnp.bfloat16, jnp.float32
    mixed = pl.pallas_call(
        mixer_kernel,
        out_shape=jax.ShapeDtypeStruct((HEADS, TOK, DH), bf16),
        in_specs=[hbm, hbm, hbm, vmem, vmem],
        out_specs=vmem,
        scratch_shapes=[
            pltpu.VMEM((8 * TOK, DH), bf16),
            pltpu.VMEM((8 * TOK, DH), bf16),
            pltpu.VMEM((8 * TOK, DH), bf16),
            pltpu.VMEM((DEV, HEADS, TOK), f32),
            pltpu.VMEM((DEV, HEADS, TOK), f32),
            pltpu.VMEM((4, DH, DH), bf16),
            pltpu.VMEM((4, DH, DH), bf16),
            pltpu.VMEM((DH, DH), f32),
            pltpu.VMEM((4, 1, DH), f32),
            pltpu.VMEM((8, DH), f32),
            pltpu.VMEM((DH, DH), bf16),
            pltpu.VMEM((DH, DH), bf16),
            pltpu.VMEM((8, DH), f32),
            pltpu.VMEM((8 * TOK, DH), bf16),
            pltpu.VMEM((8, CHUNK), f32),
            pltpu.VMEM((8, CHUNK), f32),
            pltpu.VMEM((4, 1, CHUNK), f32),
            pltpu.VMEM((4, CHUNK, 8), f32),
            dma((3,)),
            dma((2, DEV)),
            dma((2, DEV)),
            dma((7,)),
            dma((8,)),
            dma((7,)),
            dma((8,)),
            dma((7,)),
            dma((8,)),
            dma((8,)),
            dma((8,)),
            dma((2,)),
            dma((2,)),
        ],
        compiler_params=pltpu.CompilerParams(
            collective_id=0, has_side_effects=True, vmem_limit_bytes=60 << 20
        ),
        name="mixer",
    )(queries, key_vectors, value_vectors, input_logit, forget_logit)
    return pl.pallas_call(
        expert_kernel,
        out_shape=jax.ShapeDtypeStruct((TOK, D), bf16),
        in_specs=[vmem] * 6 + [hbm] * 3,
        out_specs=vmem,
        scratch_shapes=[
            pltpu.VMEM((FF, D), bf16),
            pltpu.VMEM((FF, D), bf16),
            pltpu.VMEM((FF, D), bf16),
            pltpu.VMEM((DEV * CAP, D), bf16),
            pltpu.VMEM((DEV * CAP, D), bf16),
            pltpu.VMEM((DEV * CAP, D), bf16),
            pltpu.VMEM((DEV * CAP, D), bf16),
            pltpu.VMEM((TOK, D), bf16),
            pltpu.VMEM((TOK, D), bf16),
            pltpu.VMEM((4, 2 * TOK, TOK), bf16),
            pltpu.VMEM((TOK, D), f32),
            dma((3,)),
            dma((DEV,)),
            dma((DEV,)),
            dma((DEV,)),
            dma((DEV,)),
        ],
        compiler_params=pltpu.CompilerParams(
            collective_id=1, has_side_effects=True, vmem_limit_bytes=60 << 20
        ),
        name="experts",
    )(
        mixed,
        residual_in,
        mix_gain.reshape(1, D),
        ffn_gain.reshape(1, D),
        jnp.transpose(routes),
        jnp.transpose(route_weight),
        jnp.swapaxes(expert_gate[0], 0, 1),
        jnp.swapaxes(expert_up[0], 0, 1),
        expert_down[0],
    )


def solution(mesh):
    return jax.shard_map(
        shards,
        mesh=mesh,
        in_specs=(
            P(("batch", "seq"), None),
            P(("batch", "seq"), None),
            P(("batch", "seq"), None),
            P(("batch", "seq"), None),
            P(None, ("batch", "seq")),
            P(None, ("batch", "seq")),
            P(),
            P(),
            P("seq", None, None),
            P("seq", None, None),
            P("seq", None, None),
            P(("batch", "seq"), None),
            P(("batch", "seq"), None),
        ),
        out_specs=P(("batch", "seq"), None),
        check_vma=False,
    )
```

```python
import functools
import math

import jax
import jax.numpy as jnp
from jax import lax
from jax.experimental import pallas as pl
from jax.experimental.pallas import tpu as pltpu
from jax.sharding import PartitionSpec as P

NEG_FILL = -1e30
EPSILON = 1e-06
MESH = pl.DeviceIdType.MESH
HEADS = 8
DH = 512
D = 4096
FF = 704
TOK = 128
CAP = 32
DEV = 16
CHUNK = 256
ROOT = 1.0 / math.sqrt(DH)
ORDER = (0, 1, 3, 4, 12, 2, 8, 10, 5, 15, 7, 13, 6, 14, 9, 11)
NEAR = ((0, 1), (0, 3), (1, 0), (1, 1), (1, 3), (0, 2), (1, 2))


def peer_of(me, offset):
    row = lax.rem(me // 4 + offset // 4, 4)
    col = lax.rem(lax.rem(me, 4) + offset % 4, 4)
    return row * 4 + col


def entry_barrier(me):
    barrier = pltpu.get_barrier_semaphore()
    for offset in range(1, DEV):
        pl.semaphore_signal(
            barrier, inc=1, device_id={"seq": peer_of(me, offset)}, device_id_type=MESH
        )
    pl.semaphore_wait(barrier, DEV - 1)


def remote(src, dst, send, recv, device):
    return pltpu.make_async_remote_copy(
        src_ref=src,
        dst_ref=dst,
        send_sem=send,
        recv_sem=recv,
        device_id={"seq": device},
        device_id_type=MESH,
    )


def scan_lanes(x, op, fill):
    lane = lax.broadcasted_iota(jnp.int32, x.shape, 1)
    step = 1
    while step < x.shape[1]:
        x = op(x, jnp.where(lane >= step, pltpu.roll(x, step, 1), fill))
        step *= 2
    return x


def three_parts(x):
    high = x.astype(jnp.bfloat16).astype(jnp.float32)
    rest = x - high
    middle = rest.astype(jnp.bfloat16).astype(jnp.float32)
    return high, middle, rest - middle


def nt_dot(a, b):
    return lax.dot_general(a, b, (((1,), (1,)), ((), ())), preferred_element_type=jnp.float32)


def kernel(
    q_in, k_in, v_in, gate_i, gate_f, residual_in, gain_m, gain_f, routes_in, share_in, w_gate, w_up, w_down, out,
    qb, kb, vb, kwt, gbi, gbf, chi, clo, sacc, zst, z_in, st_in, st_out, z_out, ob, mix, rowi, rowf, grow, tcol,
    residual, mix_gain, ffn_gain, routes, route_weight,
    gate_v, up_v, down_v, disp, inbox, result, back, upd, normed, picks, wmat, acc,
    own_sem, w_sem, gs, gr, ks, kr, vs, vr, qs, qr, os, orr, ss, sr, ds, dr, bs, br,
):
    me = lax.axis_index("seq")
    half = me // 8
    base = half * 8
    local = me - base
    pair = local // 2
    head = lax.rem(local + 4 * half, 8)

    def rows(j):
        return pl.ds(pl.multiple_of(j * TOK, TOK), TOK)

    def head_columns(h):
        return pl.ds(pl.multiple_of(h * DH, DH), DH)

    own = [
        pltpu.make_async_copy(src.at[:, head_columns(head)], dst, own_sem.at[n])
        for n, (src, dst) in enumerate(
            ((k_in, kb.at[rows(local), :]), (v_in, vb.at[rows(local), :]), (q_in, qb.at[rows(local), :]))
        )
    ]
    own_gates = [
        pltpu.make_async_copy(gate_i, gbi.at[me], own_sem.at[3]),
        pltpu.make_async_copy(gate_f, gbf.at[me], own_sem.at[4]),
    ]
    fetched = [
        pltpu.make_async_copy(src, dst, w_sem.at[n])
        for n, (src, dst) in enumerate(
            (
                (routes_in, routes),
                (share_in, route_weight),
                (gain_m, mix_gain),
                (gain_f, ffn_gain),
                (residual_in, residual),
                (w_gate, gate_v),
                (w_up, up_v),
                (w_down, down_v),
            )
        )
    ]
    for copy in own + own_gates + fetched:
        copy.start()
    entry_barrier(me)

    sent = []
    for offset in range(1, DEV):
        to = peer_of(me, offset)
        for src, dst, n in ((gate_i, gbi, 0), (gate_f, gbf, 1)):
            copy = remote(src, dst.at[me], gs.at[n, offset], gr.at[n, me], to)
            copy.start()
            sent.append(copy)

    def send_part(src, dst, send, recv, lo, width, to):
        to_head = lax.rem(to + 4 * half, 8)
        part = pl.ds(pl.multiple_of(to_head * DH + lo, width), width)
        copy = remote(src.at[:, part], dst.at[rows(local), lo : lo + width], send, recv, base + to)
        copy.start()
        sent.append(copy)

    for src, dst, send, recv in ((k_in, kb, ks, kr), (v_in, vb, vs, vr)):
        for part in range(2):
            for n, (dy, dx) in enumerate(NEAR):
                to = lax.rem(local // 4 + dy, 2) * 4 + lax.rem(lax.rem(local, 4) + dx, 4)
                send_part(src, dst, send.at[part, n], recv.at[part, local], part * 256, 256, to)
    for n in range(7):
        if n < 6:
            to = 2 * lax.rem(pair + 3 - n // 2, 4) + n % 2
        else:
            to = 2 * pair + 1 - lax.rem(local, 2)
        send_part(q_in, qb, qs.at[n], qr.at[local], 0, DH, to)

    for n in range(4):
        fetched[n].wait()
    owner = jnp.zeros((DEV, TOK), jnp.int32)
    row16 = lax.broadcasted_iota(jnp.int32, (DEV, TOK), 0)
    for n, offset in enumerate(ORDER):
        owner = jnp.where(row16 == n, peer_of(me, offset), owner)
    hit0 = routes[0:1, :] == owner
    hit1 = routes[1:2, :] == owner
    match = jnp.where(hit0 | hit1, 1.0, 0.0).astype(jnp.bfloat16)
    earlier = lax.broadcasted_iota(jnp.int32, (TOK, TOK), 0) < lax.broadcasted_iota(
        jnp.int32, (TOK, TOK), 1
    )
    position = jnp.dot(
        match, jnp.where(earlier, 1.0, 0.0).astype(jnp.bfloat16), preferred_element_type=jnp.float32
    )
    slot = position + (row16 * CAP).astype(jnp.float32)
    slot0 = jnp.sum(jnp.where(hit0, slot, 0.0), axis=0, keepdims=True)
    slot1 = jnp.sum(jnp.where(hit1, slot, 0.0), axis=0, keepdims=True)
    row8 = lax.broadcasted_iota(jnp.int32, (8, TOK), 0)
    packed = jnp.where(
        row8 == 0,
        slot0,
        jnp.where(row8 == 1, slot1, jnp.where(row8 == 2, route_weight[0:1, :], route_weight[1:2, :])),
    )
    columns = jnp.transpose(packed)
    lane = lax.broadcasted_iota(jnp.int32, (TOK, DEV * CAP), 1).astype(jnp.float32)
    share = jnp.where(lane == columns[:, 0:1], columns[:, 2:3], 0.0) + jnp.where(
        lane == columns[:, 1:2], columns[:, 3:4], 0.0
    )
    high = share.astype(jnp.bfloat16)
    low = (share - high.astype(jnp.float32)).astype(jnp.bfloat16)
    for g in range(4):
        wmat[g, 0:TOK, :] = high[:, g * TOK : (g + 1) * TOK]
        wmat[g, TOK : 2 * TOK, :] = low[:, g * TOK : (g + 1) * TOK]
        target = lax.broadcasted_iota(jnp.int32, (TOK, TOK), 0) + g * TOK
        pick = jnp.where((target == slot0.astype(jnp.int32)) | (target == slot1.astype(jnp.int32)), 1.0, 0.0)
        picks[g] = pick.astype(jnp.bfloat16)

    for copy in own_gates:
        copy.wait()
    for offset in range(1, DEV):
        src = peer_of(me, offset)
        remote(gate_i, gbi.at[src], gs.at[0, offset], gr.at[0, src], me).wait_recv()
        remote(gate_f, gbf.at[src], gs.at[1, offset], gr.at[1, src], me).wait_recv()
    for b in range(DEV):
        rowi[b // 2 : b // 2 + 1, (b % 2) * TOK : (b % 2 + 1) * TOK] = gbi[b, pl.ds(head, 1), :]
        rowf[b // 2 : b // 2 + 1, (b % 2) * TOK : (b % 2 + 1) * TOK] = gbf[b, pl.ds(head, 1), :]
    x = rowf[...]
    log_forget = jnp.minimum(x, 0.0) - jnp.log1p(jnp.exp(-jnp.abs(x)))
    cumul = scan_lanes(log_forget, jnp.add, 0.0)
    lift = rowi[...] - cumul
    lift_max = scan_lanes(lift, jnp.maximum, NEG_FILL)
    decay = cumul[:, CHUNK - 1 : CHUNK]
    peak_in = decay + lift_max[:, CHUNK - 1 : CHUNK]
    peaks = [jnp.full((1, 1), NEG_FILL, jnp.float32)]
    for c in range(8):
        peaks.append(jnp.maximum(decay[c : c + 1] + peaks[-1], peak_in[c : c + 1]))
    first = half == 0
    scales = []
    since = jnp.ones((1, 1), jnp.float32)
    row8 = lax.broadcasted_iota(jnp.int32, (8, CHUNK), 0)
    for c in range(4):
        before = jnp.where(first, peaks[c], peaks[4 + c])
        after = jnp.where(first, peaks[c + 1], peaks[5 + c])
        dec = jnp.where(first, decay[c : c + 1], decay[4 + c : 5 + c])
        lift_c = jnp.where(first, lift[c : c + 1], lift[4 + c : 5 + c])
        top = jnp.maximum(jnp.where(first, lift_max[c : c + 1], lift_max[4 + c : 5 + c]), before)
        weight = jnp.exp(dec + lift_c - after)
        reach = jnp.exp(before - top) * ROOT
        packed = jnp.where(
            row8 == 0, weight, jnp.where(row8 == 1, top, jnp.where(row8 == 2, reach, reach * since))
        )
        tcol[c] = jnp.transpose(packed)
        grow[c] = lift_c
        scales.append(jnp.exp(dec + before - after))
        since = since * scales[-1]

    z_now = jnp.zeros((1, DH), jnp.float32)
    for c in range(4):
        for j in (2 * c, 2 * c + 1):

            @pl.when(j != local)
            def _():
                for part in range(2):
                    piece = kb.at[rows(j), part * 256 : part * 256 + 256]
                    remote(piece, piece, ks.at[part, 0], kr.at[part, j], me).wait_recv()

            @pl.when(j == local)
            def _():
                own[0].wait()

        weighted = kb[c * CHUNK : (c + 1) * CHUNK, :].astype(jnp.float32) * tcol[c][:, 0:1]
        kwt[c] = jnp.transpose(weighted.astype(jnp.bfloat16))
        zst[c] = z_now
        z_now = scales[c] * z_now + jnp.sum(weighted, axis=0, keepdims=True)
    z_out[...] = jnp.broadcast_to(z_now, (8, DH))
    chi[0] = jnp.zeros((DH, DH), jnp.bfloat16)
    clo[0] = jnp.zeros((DH, DH), jnp.bfloat16)

    next_device = 8 + lax.rem(local + 4, 8)
    onward = [remote(z_out, z_in, ss.at[2], sr.at[2], next_device)] + [
        remote(st_out.at[part], st_in.at[part], ss.at[part], sr.at[part], next_device) for part in range(2)
    ]
    for part in range(2):
        cols = slice(part * 256, part * 256 + 256)
        for c in range(4):
            for j in (2 * c, 2 * c + 1):

                @pl.when(j != local)
                def _():
                    piece = vb.at[rows(j), cols]
                    remote(piece, piece, vs.at[part, 0], vr.at[part, j], me).wait_recv()

                if part == 0:

                    @pl.when(j == local)
                    def _():
                        own[1].wait()

            state = jnp.dot(kwt[c], vb[c * CHUNK : (c + 1) * CHUNK, cols], preferred_element_type=jnp.float32)
            if c > 0:
                state += scales[c] * sacc[...]
            high = state.astype(jnp.bfloat16)
            if c < 3:
                sacc[...] = state
                chi[c + 1, :, cols] = high
                clo[c + 1, :, cols] = (state - high.astype(jnp.float32)).astype(jnp.bfloat16)
            else:
                st_out[part] = high

        @pl.when(half == 0)
        def _():
            if part == 0:
                onward[0].start()
            onward[1 + part].start()

    @pl.when(half == 0)
    def _():
        z_in[...] = jnp.zeros((8, DH), jnp.float32)

    @pl.when(half == 1)
    def _():
        for copy in onward:
            copy.wait_recv()

    causal = lax.broadcasted_iota(jnp.int32, (CHUNK, CHUNK), 0) >= lax.broadcasted_iota(
        jnp.int32, (CHUNK, CHUNK), 1
    )
    z_row = lax.broadcasted_iota(jnp.int32, (8, DH), 0)

    @pl.loop(0, 4)
    def _(i):
        c = lax.rem(i + 1 + pair, 4)
        for jj in range(2):
            j = 2 * c + jj

            @pl.when(j != local)
            def _():
                remote(qb.at[rows(j), :], qb.at[rows(j), :], qs.at[0], qr.at[j], me).wait_recv()

            @pl.when(j == local)
            def _():
                own[2].wait()

        part = pl.ds(pl.multiple_of(c * CHUNK, CHUNK), CHUNK)
        query = qb[part, :]
        value = vb[part, :]
        columns = tcol[c]
        top, reach, reach0 = columns[:, 1:2], columns[:, 2:3], columns[:, 3:4]
        weight = jnp.exp(jnp.where(causal, grow[c] - top, NEG_FILL))
        coef = weight * (nt_dot(query, kb[part, :]) * ROOT)
        denom = jnp.sum(coef, axis=1, keepdims=True)
        numer = jnp.dot(coef.astype(jnp.bfloat16), value, preferred_element_type=jnp.float32)
        held = jnp.dot(query, chi[c], preferred_element_type=jnp.float32)
        held += jnp.dot(query, clo[c], preferred_element_type=jnp.float32)
        parts = three_parts(zst[c]) + three_parts(z_in[0:1, :])
        z_all = jnp.zeros((8, DH), jnp.float32)
        for n, piece in enumerate(parts):
            z_all = jnp.where(z_row == n, piece, z_all)
        norm = nt_dot(query, z_all.astype(jnp.bfloat16))
        denom += reach * (norm[:, 0:1] + norm[:, 1:2] + norm[:, 2:3])
        denom += reach0 * (norm[:, 3:4] + norm[:, 4:5] + norm[:, 5:6])
        numer += reach * held

        def finish(total):
            ob[part, :] = (total / jnp.maximum(jnp.abs(denom), 1.0)).astype(jnp.bfloat16)

        @pl.when(half == 0)
        def _():
            finish(numer)

        @pl.when(half == 1)
        def _():
            from_first = jnp.concatenate(
                [jnp.dot(query, st_in[n], preferred_element_type=jnp.float32) for n in range(2)], axis=1
            )
            finish(numer + reach0 * from_first)

        for jj in range(2):
            j = 2 * c + jj

            @pl.when(j != local)
            def _():
                remote(ob.at[rows(j), :], mix.at[head], os.at[j], orr.at[head], base + j).start()

            @pl.when(j == local)
            def _():
                mix[head] = ob[rows(j), :]

    fetched[4].wait()
    for j in range(8):

        @pl.when(j != local)
        def _():
            from_head = lax.rem(j + 4 * half, 8)
            remote(ob.at[rows(j), :], mix.at[from_head], os.at[j], orr.at[from_head], me).wait_recv()

    square = jnp.zeros((TOK, 1), jnp.float32)
    for h in range(HEADS):
        part = mix[h].astype(jnp.float32)
        square += jnp.sum(part * part, axis=1, keepdims=True)
    scale = lax.rsqrt(square * (1.0 / D) + EPSILON)
    square = jnp.zeros((TOK, 1), jnp.float32)
    for h in range(HEADS):
        cols = slice(h * DH, (h + 1) * DH)
        part = residual[:, cols].astype(jnp.float32) + mix[h].astype(jnp.float32) * scale * mix_gain[:, cols]
        rounded = part.astype(jnp.bfloat16)
        upd[:, cols] = rounded
        part = rounded.astype(jnp.float32)
        square += jnp.sum(part * part, axis=1, keepdims=True)
    scale = lax.rsqrt(square * (1.0 / D) + EPSILON)
    for h in range(HEADS):
        cols = slice(h * DH, (h + 1) * DH)
        part = upd[:, cols].astype(jnp.float32)
        acc[:, cols] = part
        normed[:, cols] = (part * scale * ffn_gain[:, cols]).astype(jnp.bfloat16)

    pieces = 4
    depth = CAP // pieces
    for g in range(4):
        for h in range(HEADS):
            cols = slice(h * DH, (h + 1) * DH)
            picked = jnp.dot(picks[g], normed[:, cols], preferred_element_type=jnp.float32)
            disp[g * TOK : (g + 1) * TOK, cols] = picked.astype(jnp.bfloat16)
        for p in range(pieces):
            for n in range(4 * g, 4 * g + 4):
                if n == 0:
                    continue
                piece = pl.ds(n * CAP + p * depth, depth)
                remote(
                    disp.at[piece, :], inbox.at[piece, :], ds.at[n], dr.at[n], peer_of(me, ORDER[n])
                ).start()
    inbox[0:CAP, :] = disp[0:CAP, :]

    def slot_rows(n):
        return pl.ds(n * CAP, CAP)

    for n in range(5, 8):
        fetched[n].wait()

    for g in range(4):
        for n in range(4 * g, 4 * g + 4):
            if n > 0:
                remote(disp.at[slot_rows(n), :], inbox.at[slot_rows(n), :], ds.at[n], dr.at[n], me).wait_recv()
        arrived = inbox[g * TOK : (g + 1) * TOK, :]
        gate = nt_dot(arrived, gate_v[...])
        up = nt_dot(arrived, up_v[...])
        hidden = (gate / (1.0 + jnp.exp(-gate)) * up).astype(jnp.bfloat16)
        for h in range(HEADS):
            cols = slice(h * DH, (h + 1) * DH)
            result[g * TOK : (g + 1) * TOK, cols] = jnp.dot(
                hidden, down_v[:, cols], preferred_element_type=jnp.float32
            ).astype(jnp.bfloat16)
        for p in range(pieces):
            for n in range(4 * g, 4 * g + 4):
                if n == 0:
                    continue
                piece = pl.ds(n * CAP + p * depth, depth)
                back_to = peer_of(me, (4 - ORDER[n] // 4) % 4 * 4 + (4 - ORDER[n] % 4) % 4)
                remote(result.at[piece, :], back.at[piece, :], bs.at[n], br.at[n], back_to).start()
    back[0:CAP, :] = result[0:CAP, :]

    for g in range(4):
        for n in range(4 * g, 4 * g + 4):
            if n > 0:
                remote(result.at[slot_rows(n), :], back.at[slot_rows(n), :], bs.at[n], br.at[n], me).wait_recv()
        for h in range(HEADS):
            cols = slice(h * DH, (h + 1) * DH)
            both = jnp.dot(wmat[g], back[g * TOK : (g + 1) * TOK, cols], preferred_element_type=jnp.float32)
            total = acc[:, cols] + both[0:TOK, :] + both[TOK : 2 * TOK, :]
            if g < 3:
                acc[:, cols] = total
            else:
                out[:, cols] = total.astype(jnp.bfloat16)

    for copy in sent:
        copy.wait_send()

    @pl.when(half == 0)
    def _():
        for copy in onward:
            copy.wait_send()

    for j in range(8):

        @pl.when(j != local)
        def _():
            remote(ob.at[rows(j), :], mix.at[j], os.at[j], orr.at[j], me).wait_send()

    for n in range(1, DEV):
        remote(disp.at[slot_rows(n), :], inbox.at[slot_rows(n), :], ds.at[n], dr.at[n], me).wait_send()
        remote(result.at[slot_rows(n), :], back.at[slot_rows(n), :], bs.at[n], br.at[n], me).wait_send()


def shards(
    queries, key_vectors, value_vectors, residual_in, input_logit, forget_logit, mix_gain, ffn_gain,
    expert_gate, expert_up, expert_down, routes, route_weight,
):
    hbm = pl.BlockSpec(memory_space=pl.ANY)
    dma = pltpu.SemaphoreType.DMA
    vmem = pltpu.VMEM
    bf16, f32 = jnp.bfloat16, jnp.float32
    return pl.pallas_call(
        kernel,
        out_shape=pltpu.VMEM((TOK, D), bf16),
        in_specs=[hbm] * 13,
        out_specs=pl.BlockSpec(memory_space=pltpu.VMEM),
        scratch_shapes=[
            vmem((8 * TOK, DH), bf16),
            vmem((8 * TOK, DH), bf16),
            vmem((8 * TOK, DH), bf16),
            vmem((4, DH, CHUNK), bf16),
            vmem((DEV, HEADS, TOK), f32),
            vmem((DEV, HEADS, TOK), f32),
            vmem((4, DH, DH), bf16),
            vmem((4, DH, DH), bf16),
            vmem((DH, DH // 2), f32),
            vmem((4, 1, DH), f32),
            vmem((8, DH), f32),
            vmem((2, DH, DH // 2), bf16),
            vmem((2, DH, DH // 2), bf16),
            vmem((8, DH), f32),
            vmem((8 * TOK, DH), bf16),
            vmem((HEADS, TOK, DH), bf16),
            vmem((8, CHUNK), f32),
            vmem((8, CHUNK), f32),
            vmem((4, 1, CHUNK), f32),
            vmem((4, CHUNK, 8), f32),
            vmem((TOK, D), bf16),
            vmem((1, D), f32),
            vmem((1, D), f32),
            vmem((2, TOK), jnp.int32),
            vmem((2, TOK), f32),
            vmem((FF, D), bf16),
            vmem((FF, D), bf16),
            vmem((FF, D), bf16),
            vmem((DEV * CAP, D), bf16),
            vmem((DEV * CAP, D), bf16),
            vmem((DEV * CAP, D), bf16),
            vmem((DEV * CAP, D), bf16),
            vmem((TOK, D), bf16),
            vmem((TOK, D), bf16),
            vmem((4, TOK, TOK), bf16),
            vmem((4, 2 * TOK, TOK), bf16),
            vmem((TOK, D), f32),
            dma((5,)),
            dma((8,)),
            dma((2, DEV)),
            dma((2, DEV)),
            dma((2, 7)),
            dma((2, 8)),
            dma((2, 7)),
            dma((2, 8)),
            dma((7,)),
            dma((8,)),
            dma((8,)),
            dma((8,)),
            dma((3,)),
            dma((3,)),
            dma((DEV,)),
            dma((DEV,)),
            dma((DEV,)),
            dma((DEV,)),
        ],
        compiler_params=pltpu.CompilerParams(
            collective_id=0, has_side_effects=True, vmem_limit_bytes=62 << 20
        ),
        name="block",
    )(
        queries,
        key_vectors,
        value_vectors,
        input_logit,
        forget_logit,
        residual_in,
        mix_gain.reshape(1, D),
        ffn_gain.reshape(1, D),
        jnp.transpose(routes),
        jnp.transpose(route_weight),
        jnp.swapaxes(expert_gate[0], 0, 1),
        jnp.swapaxes(expert_up[0], 0, 1),
        expert_down[0],
    )


def solution(mesh):
    return jax.shard_map(
        shards,
        mesh=mesh,
        in_specs=(
            P(("batch", "seq"), None),
            P(("batch", "seq"), None),
            P(("batch", "seq"), None),
            P(("batch", "seq"), None),
            P(None, ("batch", "seq")),
            P(None, ("batch", "seq")),
            P(),
            P(),
            P("seq", None, None),
            P("seq", None, None),
            P("seq", None, None),
            P(("batch", "seq"), None),
            P(("batch", "seq"), None),
        ),
        out_specs=P(("batch", "seq"), None),
        check_vma=False,
    )
```

```python
import functools
import math

import jax
import jax.numpy as jnp
from jax import lax
from jax.experimental import pallas as pl
from jax.experimental.pallas import tpu as pltpu
from jax.sharding import PartitionSpec as P

NEG_FILL = -1e30
EPSILON = 1e-06
MESH = pl.DeviceIdType.MESH
HEADS = 8
DH = 512
D = 4096
FF = 704
TOK = 128
CAP = 32
DEV = 16
CHUNK = 256
ROOT = 1.0 / math.sqrt(DH)
ORDER = (5, 15, 7, 13, 6, 14, 9, 11, 10, 2, 8, 12, 0, 1, 3, 4)
SELF = ORDER.index(0)
NEAR = ((0, 1), (0, 3), (1, 0), (1, 1), (1, 3), (0, 2), (1, 2))


def peer_of(me, offset):
    row = lax.rem(me // 4 + offset // 4, 4)
    col = lax.rem(lax.rem(me, 4) + offset % 4, 4)
    return row * 4 + col


def entry_barrier(me):
    barrier = pltpu.get_barrier_semaphore()
    for offset in range(1, DEV):
        pl.semaphore_signal(
            barrier, inc=1, device_id={"seq": peer_of(me, offset)}, device_id_type=MESH
        )
    pl.semaphore_wait(barrier, DEV - 1)


def remote(src, dst, send, recv, device):
    return pltpu.make_async_remote_copy(
        src_ref=src,
        dst_ref=dst,
        send_sem=send,
        recv_sem=recv,
        device_id={"seq": device},
        device_id_type=MESH,
    )


def settled(ref, semaphore):
    pltpu.make_async_copy(ref, ref, semaphore).wait()


def scan_lanes(x, op, fill):
    lane = lax.broadcasted_iota(jnp.int32, x.shape, 1)
    step = 1
    while step < x.shape[1]:
        x = op(x, jnp.where(lane >= step, pltpu.roll(x, step, 1), fill))
        step *= 2
    return x


def three_parts(x):
    high = x.astype(jnp.bfloat16).astype(jnp.float32)
    rest = x - high
    middle = rest.astype(jnp.bfloat16).astype(jnp.float32)
    return high, middle, rest - middle


def nt_dot(a, b):
    return lax.dot_general(a, b, (((1,), (1,)), ((), ())), preferred_element_type=jnp.float32)


def kernel(
    q_in, k_in, v_in, gate_i, gate_f, residual_in, gain_m, gain_f, routes_in, share_in, w_gate, w_up, w_down, out,
    qb, kb, vb, kwt, gbi, gbf, chi, clo, sacc, zst, z_in, st_in, st_out, z_out, ob, mix, rowi, rowf, grow, tcol,
    residual, mix_gain, ffn_gain, routes, route_weight,
    gate_v, up_v, down_v, disp, inbox, result, back, upd, normed, picks, wmat, acc,
    own_sem, w_sem, gs, gr, hs, hr, qr, orr, ss, sr, dr, br,
):
    me = lax.axis_index("seq")
    half = me // 8
    base = half * 8
    local = me - base
    pair = local // 2
    head = lax.rem(local + 4 * half, 8)

    def rows(j):
        return pl.ds(pl.multiple_of(j * TOK, TOK), TOK)

    def head_columns(h):
        return pl.ds(pl.multiple_of(h * DH, DH), DH)

    own = [
        pltpu.make_async_copy(src.at[:, head_columns(head)], dst, own_sem.at[n])
        for n, (src, dst) in enumerate(
            ((k_in, kb.at[rows(local), :]), (v_in, vb.at[rows(local), :]), (q_in, qb.at[rows(local), :]))
        )
    ]
    own_gates = [
        pltpu.make_async_copy(gate_i, gbi.at[me], own_sem.at[3]),
        pltpu.make_async_copy(gate_f, gbf.at[me], own_sem.at[4]),
    ]
    fetched = [
        pltpu.make_async_copy(src, dst, w_sem.at[n])
        for n, (src, dst) in enumerate(
            (
                (routes_in, routes),
                (share_in, route_weight),
                (gain_m, mix_gain),
                (gain_f, ffn_gain),
                (residual_in, residual),
                (w_gate, gate_v),
                (w_up, up_v),
                (w_down, down_v),
            )
        )
    ]
    for copy in own + own_gates + fetched:
        copy.start()
    entry_barrier(me)

    for offset in range(1, DEV):
        to = peer_of(me, offset)
        for src, dst, n in ((gate_i, gbi, 0), (gate_f, gbf, 1)):
            remote(src, dst.at[me], gs.at[n], gr.at[n], to).start()

    def send_part(src, dst, send, recv, lo, width, to):
        to_head = lax.rem(to + 4 * half, 8)
        part = pl.ds(pl.multiple_of(to_head * DH + lo, width), width)
        remote(src.at[:, part], dst.at[rows(local), lo : lo + width], send, recv, base + to).start()

    for src, dst, k in ((k_in, kb, 0), (v_in, vb, 1)):
        for part in range(2):
            for dy, dx in NEAR:
                to = lax.rem(local // 4 + dy, 2) * 4 + lax.rem(lax.rem(local, 4) + dx, 4)
                send_part(src, dst, hs.at[k], hr.at[2 * k + part], part * 256, 256, to)
    for n in range(7):
        if n < 6:
            to = 2 * lax.rem(pair + 3 - n // 2, 4) + n % 2
        else:
            to = 2 * pair + 1 - lax.rem(local, 2)
        send_part(q_in, qb, hs.at[2], qr.at[local], 0, DH, to)

    for n in range(4):
        fetched[n].wait()
    owner = jnp.zeros((DEV, TOK), jnp.int32)
    row16 = lax.broadcasted_iota(jnp.int32, (DEV, TOK), 0)
    for n, offset in enumerate(ORDER):
        owner = jnp.where(row16 == n, peer_of(me, offset), owner)
    hit0 = routes[0:1, :] == owner
    hit1 = routes[1:2, :] == owner
    match = jnp.where(hit0 | hit1, 1.0, 0.0).astype(jnp.bfloat16)
    earlier = lax.broadcasted_iota(jnp.int32, (TOK, TOK), 0) < lax.broadcasted_iota(
        jnp.int32, (TOK, TOK), 1
    )
    position = jnp.dot(
        match, jnp.where(earlier, 1.0, 0.0).astype(jnp.bfloat16), preferred_element_type=jnp.float32
    )
    slot = position + (row16 * CAP).astype(jnp.float32)
    slot0 = jnp.sum(jnp.where(hit0, slot, 0.0), axis=0, keepdims=True)
    slot1 = jnp.sum(jnp.where(hit1, slot, 0.0), axis=0, keepdims=True)
    row8 = lax.broadcasted_iota(jnp.int32, (8, TOK), 0)
    packed = jnp.where(
        row8 == 0,
        slot0,
        jnp.where(row8 == 1, slot1, jnp.where(row8 == 2, route_weight[0:1, :], route_weight[1:2, :])),
    )
    columns = jnp.transpose(packed)
    lane = lax.broadcasted_iota(jnp.int32, (TOK, DEV * CAP), 1).astype(jnp.float32)
    share = jnp.where(lane == columns[:, 0:1], columns[:, 2:3], 0.0) + jnp.where(
        lane == columns[:, 1:2], columns[:, 3:4], 0.0
    )
    high = share.astype(jnp.bfloat16)
    low = (share - high.astype(jnp.float32)).astype(jnp.bfloat16)
    for g in range(4):
        wmat[g, 0:TOK, :] = high[:, g * TOK : (g + 1) * TOK]
        wmat[g, TOK : 2 * TOK, :] = low[:, g * TOK : (g + 1) * TOK]
        target = lax.broadcasted_iota(jnp.int32, (TOK, TOK), 0) + g * TOK
        pick = jnp.where((target == slot0.astype(jnp.int32)) | (target == slot1.astype(jnp.int32)), 1.0, 0.0)
        picks[g] = pick.astype(jnp.bfloat16)

    for copy in own_gates:
        copy.wait()
    for n, ref in ((0, gbi), (1, gbf)):
        settled(ref.at[0 : DEV - 1], gr.at[n])
    for b in range(DEV):
        rowi[b // 2 : b // 2 + 1, (b % 2) * TOK : (b % 2 + 1) * TOK] = gbi[b, pl.ds(head, 1), :]
        rowf[b // 2 : b // 2 + 1, (b % 2) * TOK : (b % 2 + 1) * TOK] = gbf[b, pl.ds(head, 1), :]
    x = rowf[...]
    log_forget = jnp.minimum(x, 0.0) - jnp.log1p(jnp.exp(-jnp.abs(x)))
    cumul = scan_lanes(log_forget, jnp.add, 0.0)
    lift = rowi[...] - cumul
    lift_max = scan_lanes(lift, jnp.maximum, NEG_FILL)
    decay = cumul[:, CHUNK - 1 : CHUNK]
    peak_in = decay + lift_max[:, CHUNK - 1 : CHUNK]
    peaks = [jnp.full((1, 1), NEG_FILL, jnp.float32)]
    for c in range(8):
        peaks.append(jnp.maximum(decay[c : c + 1] + peaks[-1], peak_in[c : c + 1]))
    first = half == 0
    scales = []
    since = jnp.ones((1, 1), jnp.float32)
    row8 = lax.broadcasted_iota(jnp.int32, (8, CHUNK), 0)
    for c in range(4):
        before = jnp.where(first, peaks[c], peaks[4 + c])
        after = jnp.where(first, peaks[c + 1], peaks[5 + c])
        dec = jnp.where(first, decay[c : c + 1], decay[4 + c : 5 + c])
        lift_c = jnp.where(first, lift[c : c + 1], lift[4 + c : 5 + c])
        top = jnp.maximum(jnp.where(first, lift_max[c : c + 1], lift_max[4 + c : 5 + c]), before)
        weight = jnp.exp(dec + lift_c - after)
        reach = jnp.exp(before - top) * ROOT
        packed = jnp.where(
            row8 == 0, weight, jnp.where(row8 == 1, top, jnp.where(row8 == 2, reach, reach * since))
        )
        tcol[c] = jnp.transpose(packed)
        grow[c] = lift_c
        scales.append(jnp.exp(dec + before - after))
        since = since * scales[-1]

    z_now = jnp.zeros((1, DH), jnp.float32)
    own[0].wait()
    own[1].wait()
    for part in range(2):
        settled(kb.at[0 : 7 * TOK, part * 256 : part * 256 + 256], hr.at[part])
    for c in range(4):
        weighted = kb[c * CHUNK : (c + 1) * CHUNK, :].astype(jnp.float32) * tcol[c][:, 0:1]
        kwt[c] = jnp.transpose(weighted.astype(jnp.bfloat16))
        zst[c] = z_now
        z_now = scales[c] * z_now + jnp.sum(weighted, axis=0, keepdims=True)
    z_out[...] = jnp.broadcast_to(z_now, (8, DH))
    chi[0] = jnp.zeros((DH, DH), jnp.bfloat16)
    clo[0] = jnp.zeros((DH, DH), jnp.bfloat16)

    next_device = 8 + lax.rem(local + 4, 8)
    onward = [remote(z_out, z_in, ss.at[2], sr.at[2], next_device)] + [
        remote(st_out.at[part], st_in.at[part], ss.at[part], sr.at[part], next_device) for part in range(2)
    ]
    for part in range(2):
        cols = slice(part * 256, part * 256 + 256)
        settled(vb.at[0 : 7 * TOK, cols], hr.at[2 + part])
        for c in range(4):
            state = jnp.dot(kwt[c], vb[c * CHUNK : (c + 1) * CHUNK, cols], preferred_element_type=jnp.float32)
            if c > 0:
                state += scales[c] * sacc[...]
            high = state.astype(jnp.bfloat16)
            if c < 3:
                sacc[...] = state
                chi[c + 1, :, cols] = high
                clo[c + 1, :, cols] = (state - high.astype(jnp.float32)).astype(jnp.bfloat16)
            else:
                st_out[part] = high

        @pl.when(half == 0)
        def _():
            if part == 0:
                onward[0].start()
            onward[1 + part].start()

    @pl.when(half == 0)
    def _():
        z_in[...] = jnp.zeros((8, DH), jnp.float32)

    @pl.when(half == 1)
    def _():
        for copy in onward:
            copy.wait_recv()

    causal = lax.broadcasted_iota(jnp.int32, (CHUNK, CHUNK), 0) >= lax.broadcasted_iota(
        jnp.int32, (CHUNK, CHUNK), 1
    )
    z_row = lax.broadcasted_iota(jnp.int32, (8, DH), 0)

    @pl.loop(0, 4)
    def _(i):
        c = lax.rem(i + 1 + pair, 4)
        for jj in range(2):
            j = 2 * c + jj

            @pl.when(j != local)
            def _():
                settled(qb.at[rows(j), :], qr.at[j])

            @pl.when(j == local)
            def _():
                own[2].wait()

        part = pl.ds(pl.multiple_of(c * CHUNK, CHUNK), CHUNK)
        query = qb[part, :]
        value = vb[part, :]
        columns = tcol[c]
        top, reach, reach0 = columns[:, 1:2], columns[:, 2:3], columns[:, 3:4]
        weight = jnp.exp(jnp.where(causal, grow[c] - top, NEG_FILL))
        coef = weight * (nt_dot(query, kb[part, :]) * ROOT)
        denom = jnp.sum(coef, axis=1, keepdims=True)
        numer = jnp.dot(coef.astype(jnp.bfloat16), value, preferred_element_type=jnp.float32)
        held = jnp.dot(query, chi[c], preferred_element_type=jnp.float32)
        held += jnp.dot(query, clo[c], preferred_element_type=jnp.float32)
        parts = three_parts(zst[c]) + three_parts(z_in[0:1, :])
        z_all = jnp.zeros((8, DH), jnp.float32)
        for n, piece in enumerate(parts):
            z_all = jnp.where(z_row == n, piece, z_all)
        norm = nt_dot(query, z_all.astype(jnp.bfloat16))
        denom += reach * (norm[:, 0:1] + norm[:, 1:2] + norm[:, 2:3])
        denom += reach0 * (norm[:, 3:4] + norm[:, 4:5] + norm[:, 5:6])
        numer += reach * held

        def finish(total):
            ob[part, :] = (total / jnp.maximum(jnp.abs(denom), 1.0)).astype(jnp.bfloat16)

        @pl.when(half == 0)
        def _():
            finish(numer)

        @pl.when(half == 1)
        def _():
            from_first = jnp.concatenate(
                [jnp.dot(query, st_in[n], preferred_element_type=jnp.float32) for n in range(2)], axis=1
            )
            finish(numer + reach0 * from_first)

        for jj in range(2):
            j = 2 * c + jj

            @pl.when(j != local)
            def _():
                remote(ob.at[rows(j), :], mix.at[head], hs.at[3], orr.at[0], base + j).start()

            @pl.when(j == local)
            def _():
                mix[head] = ob[rows(j), :]

    fetched[4].wait()
    settled(mix.at[0:7], orr.at[0])
    square = jnp.zeros((TOK, 1), jnp.float32)
    for h in range(HEADS):
        part = mix[h].astype(jnp.float32)
        square += jnp.sum(part * part, axis=1, keepdims=True)
    scale = lax.rsqrt(square * (1.0 / D) + EPSILON)
    square = jnp.zeros((TOK, 1), jnp.float32)
    for h in range(HEADS):
        cols = slice(h * DH, (h + 1) * DH)
        part = residual[:, cols].astype(jnp.float32) + mix[h].astype(jnp.float32) * scale * mix_gain[:, cols]
        rounded = part.astype(jnp.bfloat16)
        upd[:, cols] = rounded
        part = rounded.astype(jnp.float32)
        square += jnp.sum(part * part, axis=1, keepdims=True)
    scale = lax.rsqrt(square * (1.0 / D) + EPSILON)
    for h in range(HEADS):
        cols = slice(h * DH, (h + 1) * DH)
        part = upd[:, cols].astype(jnp.float32)
        acc[:, cols] = part
        normed[:, cols] = (part * scale * ffn_gain[:, cols]).astype(jnp.bfloat16)

    pieces = 4
    depth = CAP // pieces
    for g in range(4):
        for h in range(HEADS):
            cols = slice(h * DH, (h + 1) * DH)
            picked = jnp.dot(picks[g], normed[:, cols], preferred_element_type=jnp.float32)
            disp[g * TOK : (g + 1) * TOK, cols] = picked.astype(jnp.bfloat16)
        for p in range(pieces):
            for n in range(4 * g, 4 * g + 4):
                if n == SELF:
                    continue
                piece = pl.ds(n * CAP + p * depth, depth)
                remote(
                    disp.at[piece, :], inbox.at[piece, :], hs.at[4], dr.at[g], peer_of(me, ORDER[n])
                ).start()
    inbox[SELF * CAP : (SELF + 1) * CAP, :] = disp[SELF * CAP : (SELF + 1) * CAP, :]

    def group_rows(g):
        return pl.ds(g * TOK, TOK - CAP if SELF // 4 == g else TOK)

    for n in range(5, 8):
        fetched[n].wait()

    for g in range(4):
        settled(inbox.at[group_rows(g), :], dr.at[g])
        arrived = inbox[g * TOK : (g + 1) * TOK, :]
        gate = nt_dot(arrived, gate_v[...])
        up = nt_dot(arrived, up_v[...])
        hidden = (gate / (1.0 + jnp.exp(-gate)) * up).astype(jnp.bfloat16)
        for h in range(HEADS):
            cols = slice(h * DH, (h + 1) * DH)
            result[g * TOK : (g + 1) * TOK, cols] = jnp.dot(
                hidden, down_v[:, cols], preferred_element_type=jnp.float32
            ).astype(jnp.bfloat16)
        for p in range(pieces):
            for n in range(4 * g, 4 * g + 4):
                if n == SELF:
                    continue
                piece = pl.ds(n * CAP + p * depth, depth)
                back_to = peer_of(me, (4 - ORDER[n] // 4) % 4 * 4 + (4 - ORDER[n] % 4) % 4)
                remote(result.at[piece, :], back.at[piece, :], hs.at[5], br.at[g], back_to).start()
    back[SELF * CAP : (SELF + 1) * CAP, :] = result[SELF * CAP : (SELF + 1) * CAP, :]

    for g in range(4):
        settled(back.at[group_rows(g), :], br.at[g])
        for h in range(HEADS):
            cols = slice(h * DH, (h + 1) * DH)
            both = jnp.dot(wmat[g], back[g * TOK : (g + 1) * TOK, cols], preferred_element_type=jnp.float32)
            total = acc[:, cols] + both[0:TOK, :] + both[TOK : 2 * TOK, :]
            if g < 3:
                acc[:, cols] = total
            else:
                out[:, cols] = total.astype(jnp.bfloat16)

    for n, ref in ((0, gbi), (1, gbf)):
        settled(ref.at[0 : DEV - 1], gs.at[n])
    for n, ref in ((0, kb), (1, vb), (2, qb), (3, ob)):
        settled(ref.at[0 : 7 * TOK, :], hs.at[n])
    for n, ref in ((4, disp), (5, result)):
        settled(ref.at[0 : (DEV - 1) * CAP, :], hs.at[n])

    @pl.when(half == 0)
    def _():
        for copy in onward:
            copy.wait_send()


def shards(
    queries, key_vectors, value_vectors, residual_in, input_logit, forget_logit, mix_gain, ffn_gain,
    expert_gate, expert_up, expert_down, routes, route_weight,
):
    hbm = pl.BlockSpec(memory_space=pl.ANY)
    dma = pltpu.SemaphoreType.DMA
    vmem = pltpu.VMEM
    bf16, f32 = jnp.bfloat16, jnp.float32
    return pl.pallas_call(
        kernel,
        out_shape=pltpu.VMEM((TOK, D), bf16),
        in_specs=[hbm] * 13,
        out_specs=pl.BlockSpec(memory_space=pltpu.VMEM),
        scratch_shapes=[
            vmem((8 * TOK, DH), bf16),
            vmem((8 * TOK, DH), bf16),
            vmem((8 * TOK, DH), bf16),
            vmem((4, DH, CHUNK), bf16),
            vmem((DEV, HEADS, TOK), f32),
            vmem((DEV, HEADS, TOK), f32),
            vmem((4, DH, DH), bf16),
            vmem((4, DH, DH), bf16),
            vmem((DH, DH // 2), f32),
            vmem((4, 1, DH), f32),
            vmem((8, DH), f32),
            vmem((2, DH, DH // 2), bf16),
            vmem((2, DH, DH // 2), bf16),
            vmem((8, DH), f32),
            vmem((8 * TOK, DH), bf16),
            vmem((HEADS, TOK, DH), bf16),
            vmem((8, CHUNK), f32),
            vmem((8, CHUNK), f32),
            vmem((4, 1, CHUNK), f32),
            vmem((4, CHUNK, 8), f32),
            vmem((TOK, D), bf16),
            vmem((1, D), f32),
            vmem((1, D), f32),
            vmem((2, TOK), jnp.int32),
            vmem((2, TOK), f32),
            vmem((FF, D), bf16),
            vmem((FF, D), bf16),
            vmem((FF, D), bf16),
            vmem((DEV * CAP, D), bf16),
            vmem((DEV * CAP, D), bf16),
            vmem((DEV * CAP, D), bf16),
            vmem((DEV * CAP, D), bf16),
            vmem((TOK, D), bf16),
            vmem((TOK, D), bf16),
            vmem((4, TOK, TOK), bf16),
            vmem((4, 2 * TOK, TOK), bf16),
            vmem((TOK, D), f32),
            dma((5,)),
            dma((8,)),
            dma((2,)),
            dma((2,)),
            dma((6,)),
            dma((4,)),
            dma((8,)),
            dma((1,)),
            dma((3,)),
            dma((3,)),
            dma((4,)),
            dma((4,)),
        ],
        compiler_params=pltpu.CompilerParams(
            collective_id=0, has_side_effects=True, vmem_limit_bytes=62 << 20
        ),
        name="block",
    )(
        queries,
        key_vectors,
        value_vectors,
        input_logit,
        forget_logit,
        residual_in,
        mix_gain.reshape(1, D),
        ffn_gain.reshape(1, D),
        jnp.transpose(routes),
        jnp.transpose(route_weight),
        jnp.swapaxes(expert_gate[0], 0, 1),
        jnp.swapaxes(expert_up[0], 0, 1),
        expert_down[0],
    )


def solution(mesh):
    return jax.shard_map(
        shards,
        mesh=mesh,
        in_specs=(
            P(("batch", "seq"), None),
            P(("batch", "seq"), None),
            P(("batch", "seq"), None),
            P(("batch", "seq"), None),
            P(None, ("batch", "seq")),
            P(None, ("batch", "seq")),
            P(),
            P(),
            P("seq", None, None),
            P("seq", None, None),
            P("seq", None, None),
            P(("batch", "seq"), None),
            P(("batch", "seq"), None),
        ),
        out_specs=P(("batch", "seq"), None),
        check_vma=False,
    )
```

```python
import functools
import math

import jax
import jax.numpy as jnp
from jax import lax
from jax.experimental import pallas as pl
from jax.experimental.pallas import tpu as pltpu
from jax.sharding import PartitionSpec as P

NEG_FILL = -1e30
EPSILON = 1e-06
MESH = pl.DeviceIdType.MESH
HEADS = 8
DH = 512
D = 4096
FF = 704
TOK = 128
CAP = 32
DEV = 16
CHUNK = 256
ROOT = 1.0 / math.sqrt(DH)
ORDER = (5, 15, 7, 13, 6, 14, 9, 11, 10, 2, 8, 12, 0, 1, 3, 4)
SELF = ORDER.index(0)
WIDE = D // 2
NEAR = ((0, 1), (0, 3), (1, 0), (1, 1), (1, 3), (0, 2), (1, 2))


def peer_of(me, offset):
    row = lax.rem(me // 4 + offset // 4, 4)
    col = lax.rem(lax.rem(me, 4) + offset % 4, 4)
    return row * 4 + col


def entry_barrier(me):
    barrier = pltpu.get_barrier_semaphore()
    for offset in range(1, DEV):
        pl.semaphore_signal(
            barrier, inc=1, device_id={"seq": peer_of(me, offset)}, device_id_type=MESH
        )
    pl.semaphore_wait(barrier, DEV - 1)


def remote(src, dst, send, recv, device):
    return pltpu.make_async_remote_copy(
        src_ref=src,
        dst_ref=dst,
        send_sem=send,
        recv_sem=recv,
        device_id={"seq": device},
        device_id_type=MESH,
    )


def settled(ref, semaphore):
    pltpu.make_async_copy(ref, ref, semaphore).wait()


def scan_lanes(x, op, fill):
    lane = lax.broadcasted_iota(jnp.int32, x.shape, 1)
    step = 1
    while step < x.shape[1]:
        x = op(x, jnp.where(lane >= step, pltpu.roll(x, step, 1), fill))
        step *= 2
    return x


def three_parts(x):
    high = x.astype(jnp.bfloat16).astype(jnp.float32)
    rest = x - high
    middle = rest.astype(jnp.bfloat16).astype(jnp.float32)
    return high, middle, rest - middle


def nt_dot(a, b):
    return lax.dot_general(a, b, (((1,), (1,)), ((), ())), preferred_element_type=jnp.float32)


def kernel(
    q_in, k_in, v_in, gate_i, gate_f, residual_in, gain_m, gain_f, routes_in, share_in, w_gate, w_up, w_down, out,
    qb, kb, vb, kwt, gbi, gbf, chi, clo, sacc, zst, z_in, st_in, st_out, z_out, ob, mix, rowi, rowf, grow, tcol,
    residual, mix_gain, ffn_gain, routes, route_weight,
    gate_v, up_v, down_v, disp, inbox, result, back, upd, normed, picks, wmat, acc, rb, mates,
    own_sem, w_sem, gs, gr, hs, hr, qr, orr, ss, sr, dr, br, fr, ar, sr2,
):
    me = lax.axis_index("seq")
    half = me // 8
    base = half * 8
    local = me - base
    pair = local // 2
    head = lax.rem(local + 4 * half, 8)

    def rows(j):
        return pl.ds(pl.multiple_of(j * TOK, TOK), TOK)

    def head_columns(h):
        return pl.ds(pl.multiple_of(h * DH, DH), DH)

    own = [
        pltpu.make_async_copy(src.at[:, head_columns(head)], dst, own_sem.at[n])
        for n, (src, dst) in enumerate(
            ((k_in, kb.at[rows(local), :]), (v_in, vb.at[rows(local), :]), (q_in, qb.at[rows(local), :]))
        )
    ]
    own_gates = [
        pltpu.make_async_copy(gate_i, gbi.at[me], own_sem.at[3]),
        pltpu.make_async_copy(gate_f, gbf.at[me], own_sem.at[4]),
    ]
    fetched = [
        pltpu.make_async_copy(src, dst, w_sem.at[n])
        for n, (src, dst) in enumerate(
            (
                (routes_in, routes),
                (share_in, route_weight),
                (gain_m, mix_gain),
                (gain_f, ffn_gain),
                (residual_in, residual),
                (w_gate, gate_v),
                (w_up, up_v),
                (w_down, down_v),
            )
        )
    ]
    for copy in own + own_gates + fetched:
        copy.start()
    entry_barrier(me)

    for offset in range(1, DEV):
        to = peer_of(me, offset)
        for src, dst, n in ((gate_i, gbi, 0), (gate_f, gbf, 1)):
            remote(src, dst.at[me], gs.at[n], gr.at[n], to).start()

    def along(axis, d):
        return peer_of(me, d if axis == 0 else 4 * d)

    for axis in range(2):
        for d in range(1, 4):
            remote(routes_in, mates.at[me], gs.at[2], gr.at[2], along(axis, d)).start()

    def send_part(src, dst, send, recv, lo, width, to):
        to_head = lax.rem(to + 4 * half, 8)
        part = pl.ds(pl.multiple_of(to_head * DH + lo, width), width)
        remote(src.at[:, part], dst.at[rows(local), lo : lo + width], send, recv, base + to).start()

    for src, dst, k in ((k_in, kb, 0), (v_in, vb, 1)):
        for part in range(2):
            for dy, dx in NEAR:
                to = lax.rem(local // 4 + dy, 2) * 4 + lax.rem(lax.rem(local, 4) + dx, 4)
                send_part(src, dst, hs.at[k], hr.at[2 * k + part], part * 256, 256, to)
    for n in range(7):
        if n < 6:
            to = 2 * lax.rem(pair + 3 - n // 2, 4) + n % 2
        else:
            to = 2 * pair + 1 - lax.rem(local, 2)
        send_part(q_in, qb, hs.at[2], qr.at[local], 0, DH, to)

    for n in range(4):
        fetched[n].wait()
    owner = jnp.zeros((DEV, TOK), jnp.int32)
    row16 = lax.broadcasted_iota(jnp.int32, (DEV, TOK), 0)
    for n, offset in enumerate(ORDER):
        owner = jnp.where(row16 == n, peer_of(me, offset), owner)
    hit0 = routes[0:1, :] == owner
    hit1 = routes[1:2, :] == owner
    match = jnp.where(hit0 | hit1, 1.0, 0.0).astype(jnp.bfloat16)
    earlier = lax.broadcasted_iota(jnp.int32, (TOK, TOK), 0) < lax.broadcasted_iota(
        jnp.int32, (TOK, TOK), 1
    )
    position = jnp.dot(
        match, jnp.where(earlier, 1.0, 0.0).astype(jnp.bfloat16), preferred_element_type=jnp.float32
    )
    slot = position + (row16 * CAP).astype(jnp.float32)
    slot0 = jnp.sum(jnp.where(hit0, slot, 0.0), axis=0, keepdims=True)
    slot1 = jnp.sum(jnp.where(hit1, slot, 0.0), axis=0, keepdims=True)
    row8 = lax.broadcasted_iota(jnp.int32, (8, TOK), 0)
    packed = jnp.where(
        row8 == 0,
        slot0,
        jnp.where(row8 == 1, slot1, jnp.where(row8 == 2, route_weight[0:1, :], route_weight[1:2, :])),
    )
    columns = jnp.transpose(packed)
    lane = lax.broadcasted_iota(jnp.int32, (TOK, DEV * CAP), 1).astype(jnp.float32)
    share = jnp.where(lane == columns[:, 0:1], columns[:, 2:3], 0.0) + jnp.where(
        lane == columns[:, 1:2], columns[:, 3:4], 0.0
    )
    high = share.astype(jnp.bfloat16)
    low = (share - high.astype(jnp.float32)).astype(jnp.bfloat16)
    for g in range(4):
        wmat[g, 0:TOK, :] = high[:, g * TOK : (g + 1) * TOK]
        wmat[g, TOK : 2 * TOK, :] = low[:, g * TOK : (g + 1) * TOK]

    settled(mates.at[0:6], gr.at[2])
    target = lax.broadcasted_iota(jnp.int32, (TOK, TOK), 0).astype(jnp.float32)
    upper = jnp.where(earlier, 1.0, 0.0).astype(jnp.bfloat16)
    for axis in range(2):
        owner = jnp.full((DEV, TOK), -1, jnp.int32)
        for t in range(4):
            owner = jnp.where(row16 == t, along(1 - axis, t), owner)
        for d in range(4):
            named = routes[...] if d == 0 else mates[along(axis, d)]
            hit0 = named[0:1, :] == owner
            hit1 = named[1:2, :] == owner
            match = jnp.where(hit0 | hit1, 1.0, 0.0).astype(jnp.bfloat16)
            slot = jnp.dot(match, upper, preferred_element_type=jnp.float32) + (row16 * CAP + 1).astype(jnp.float32)
            slot0 = jnp.sum(jnp.where(hit0, slot, 0.0), axis=0, keepdims=True) - 1.0
            slot1 = jnp.sum(jnp.where(hit1, slot, 0.0), axis=0, keepdims=True) - 1.0
            pick = jnp.where((target == slot0) | (target == slot1), 1.0, 0.0)
            picks[axis, d] = pick.astype(jnp.bfloat16)

    for copy in own_gates:
        copy.wait()
    for n, ref in ((0, gbi), (1, gbf)):
        settled(ref.at[0 : DEV - 1], gr.at[n])
    for b in range(DEV):
        rowi[b // 2 : b // 2 + 1, (b % 2) * TOK : (b % 2 + 1) * TOK] = gbi[b, pl.ds(head, 1), :]
        rowf[b // 2 : b // 2 + 1, (b % 2) * TOK : (b % 2 + 1) * TOK] = gbf[b, pl.ds(head, 1), :]
    x = rowf[...]
    log_forget = jnp.minimum(x, 0.0) - jnp.log1p(jnp.exp(-jnp.abs(x)))
    cumul = scan_lanes(log_forget, jnp.add, 0.0)
    lift = rowi[...] - cumul
    lift_max = scan_lanes(lift, jnp.maximum, NEG_FILL)
    decay = cumul[:, CHUNK - 1 : CHUNK]
    peak_in = decay + lift_max[:, CHUNK - 1 : CHUNK]
    peaks = [jnp.full((1, 1), NEG_FILL, jnp.float32)]
    for c in range(8):
        peaks.append(jnp.maximum(decay[c : c + 1] + peaks[-1], peak_in[c : c + 1]))
    first = half == 0
    scales = []
    since = jnp.ones((1, 1), jnp.float32)
    row8 = lax.broadcasted_iota(jnp.int32, (8, CHUNK), 0)
    for c in range(4):
        before = jnp.where(first, peaks[c], peaks[4 + c])
        after = jnp.where(first, peaks[c + 1], peaks[5 + c])
        dec = jnp.where(first, decay[c : c + 1], decay[4 + c : 5 + c])
        lift_c = jnp.where(first, lift[c : c + 1], lift[4 + c : 5 + c])
        top = jnp.maximum(jnp.where(first, lift_max[c : c + 1], lift_max[4 + c : 5 + c]), before)
        weight = jnp.exp(dec + lift_c - after)
        reach = jnp.exp(before - top) * ROOT
        packed = jnp.where(
            row8 == 0, weight, jnp.where(row8 == 1, top, jnp.where(row8 == 2, reach, reach * since))
        )
        tcol[c] = jnp.transpose(packed)
        grow[c] = lift_c
        scales.append(jnp.exp(dec + before - after))
        since = since * scales[-1]

    z_now = jnp.zeros((1, DH), jnp.float32)
    own[0].wait()
    own[1].wait()
    for part in range(2):
        settled(kb.at[0 : 7 * TOK, part * 256 : part * 256 + 256], hr.at[part])
    for c in range(4):
        weighted = kb[c * CHUNK : (c + 1) * CHUNK, :].astype(jnp.float32) * tcol[c][:, 0:1]
        kwt[c] = jnp.transpose(weighted.astype(jnp.bfloat16))
        zst[c] = z_now
        z_now = scales[c] * z_now + jnp.sum(weighted, axis=0, keepdims=True)
    z_out[...] = jnp.broadcast_to(z_now, (8, DH))
    chi[0] = jnp.zeros((DH, DH), jnp.bfloat16)
    clo[0] = jnp.zeros((DH, DH), jnp.bfloat16)

    next_device = 8 + lax.rem(local + 4, 8)
    onward = [remote(z_out, z_in, ss.at[2], sr.at[2], next_device)] + [
        remote(st_out.at[part], st_in.at[part], ss.at[part], sr.at[part], next_device) for part in range(2)
    ]
    for part in range(2):
        cols = slice(part * 256, part * 256 + 256)
        settled(vb.at[0 : 7 * TOK, cols], hr.at[2 + part])
        for c in range(4):
            state = jnp.dot(kwt[c], vb[c * CHUNK : (c + 1) * CHUNK, cols], preferred_element_type=jnp.float32)
            if c > 0:
                state += scales[c] * sacc[...]
            high = state.astype(jnp.bfloat16)
            if c < 3:
                sacc[...] = state
                chi[c + 1, :, cols] = high
                clo[c + 1, :, cols] = (state - high.astype(jnp.float32)).astype(jnp.bfloat16)
            else:
                st_out[part] = high

        @pl.when(half == 0)
        def _():
            if part == 0:
                onward[0].start()
            onward[1 + part].start()

    @pl.when(half == 0)
    def _():
        z_in[...] = jnp.zeros((8, DH), jnp.float32)

    @pl.when(half == 1)
    def _():
        for copy in onward:
            copy.wait_recv()

    causal = lax.broadcasted_iota(jnp.int32, (CHUNK, CHUNK), 0) >= lax.broadcasted_iota(
        jnp.int32, (CHUNK, CHUNK), 1
    )
    z_row = lax.broadcasted_iota(jnp.int32, (8, DH), 0)

    @pl.loop(0, 4)
    def _(i):
        c = lax.rem(i + 1 + pair, 4)
        for jj in range(2):
            j = 2 * c + jj

            @pl.when(j != local)
            def _():
                settled(qb.at[rows(j), :], qr.at[j])

            @pl.when(j == local)
            def _():
                own[2].wait()

        part = pl.ds(pl.multiple_of(c * CHUNK, CHUNK), CHUNK)
        query = qb[part, :]
        value = vb[part, :]
        columns = tcol[c]
        top, reach, reach0 = columns[:, 1:2], columns[:, 2:3], columns[:, 3:4]
        weight = jnp.exp(jnp.where(causal, grow[c] - top, NEG_FILL))
        coef = weight * (nt_dot(query, kb[part, :]) * ROOT)
        denom = jnp.sum(coef, axis=1, keepdims=True)
        numer = jnp.dot(coef.astype(jnp.bfloat16), value, preferred_element_type=jnp.float32)
        held = jnp.dot(query, chi[c], preferred_element_type=jnp.float32)
        held += jnp.dot(query, clo[c], preferred_element_type=jnp.float32)
        parts = three_parts(zst[c]) + three_parts(z_in[0:1, :])
        z_all = jnp.zeros((8, DH), jnp.float32)
        for n, piece in enumerate(parts):
            z_all = jnp.where(z_row == n, piece, z_all)
        norm = nt_dot(query, z_all.astype(jnp.bfloat16))
        denom += reach * (norm[:, 0:1] + norm[:, 1:2] + norm[:, 2:3])
        denom += reach0 * (norm[:, 3:4] + norm[:, 4:5] + norm[:, 5:6])
        numer += reach * held

        def finish(total):
            ob[part, :] = (total / jnp.maximum(jnp.abs(denom), 1.0)).astype(jnp.bfloat16)

        @pl.when(half == 0)
        def _():
            finish(numer)

        @pl.when(half == 1)
        def _():
            from_first = jnp.concatenate(
                [jnp.dot(query, st_in[n], preferred_element_type=jnp.float32) for n in range(2)], axis=1
            )
            finish(numer + reach0 * from_first)

        for jj in range(2):
            j = 2 * c + jj

            @pl.when(j != local)
            def _():
                remote(ob.at[rows(j), :], mix.at[head], hs.at[3], orr.at[0], base + j).start()

            @pl.when(j == local)
            def _():
                mix[head] = ob[rows(j), :]

    fetched[4].wait()
    settled(mix.at[0:7], orr.at[0])
    square = jnp.zeros((TOK, 1), jnp.float32)
    for h in range(HEADS):
        part = mix[h].astype(jnp.float32)
        square += jnp.sum(part * part, axis=1, keepdims=True)
    scale = lax.rsqrt(square * (1.0 / D) + EPSILON)
    square = jnp.zeros((TOK, 1), jnp.float32)
    for h in range(HEADS):
        cols = slice(h * DH, (h + 1) * DH)
        part = residual[:, cols].astype(jnp.float32) + mix[h].astype(jnp.float32) * scale * mix_gain[:, cols]
        rounded = part.astype(jnp.bfloat16)
        upd[:, cols] = rounded
        part = rounded.astype(jnp.float32)
        square += jnp.sum(part * part, axis=1, keepdims=True)
    scale = lax.rsqrt(square * (1.0 / D) + EPSILON)
    for h in range(HEADS):
        cols = slice(h * DH, (h + 1) * DH)
        part = upd[:, cols].astype(jnp.float32)
        acc[:, cols] = part
        normed[:, cols] = (part * scale * ffn_gain[:, cols]).astype(jnp.bfloat16)

    pieces = 4
    depth = CAP // pieces

    def quarter(p):
        return slice(p * 512, p * 512 + 512)

    def gather_sems(axis, way, p):
        if p // 2 == way:
            return fr.at[axis, way, p % 2]
        return ar.at[axis, way]

    for k in range(4):
        for axis in range(2):
            for way in range(2):
                p = (k + 2 * way) % 4
                remote(
                    normed.at[:, axis * WIDE + p * 512 : axis * WIDE + p * 512 + 512],
                    rb.at[axis, 2 - 2 * way, :, quarter(p)],
                    hs.at[6],
                    gather_sems(axis, way, p),
                    along(axis, 1 + 2 * way),
                ).start()

    def block_of(axis, d, t):
        back_d = (4 - d) % 4
        return ORDER.index(t * 4 + back_d if axis == 0 else back_d * 4 + t)

    def pass_on(axis, d):
        for p in range(4):
            cols = slice(axis * WIDE + p * 512, axis * WIDE + p * 512 + 512)
            rows_here = normed[:, cols] if d == 0 else rb[axis, d - 1, :, quarter(p)]
            picked = jnp.dot(picks[axis, d], rows_here, preferred_element_type=jnp.float32)
            disp[d * TOK : (d + 1) * TOK, cols] = picked.astype(jnp.bfloat16)
        cols = slice(axis * WIDE, (axis + 1) * WIDE)
        for part in range(2):
            for t in (1, 3, 2):
                n = block_of(axis, d, t)
                remote(
                    disp.at[pl.ds(d * TOK + t * CAP + part * 16, 16), cols],
                    inbox.at[pl.ds(n * CAP + part * 16, 16), cols],
                    hs.at[4],
                    dr.at[n // 4],
                    along(1 - axis, t),
                ).start()
        n = block_of(axis, d, 0)
        inbox[n * CAP : (n + 1) * CAP, cols] = disp[d * TOK : d * TOK + CAP, cols]

    pass_on(0, 0)
    pass_on(1, 0)
    for k in range(2):
        for axis in range(2):
            for way in range(2):
                p = 2 * way + k
                came = rb.at[axis, 2 - 2 * way, :, quarter(p)]
                settled(came, fr.at[axis, way, k])
                remote(came, rb.at[axis, 1, :, quarter(p)], hs.at[6], sr2.at[axis], along(axis, 1 + 2 * way)).start()
    for axis in range(2):
        for way in range(2):
            settled(rb.at[axis, 2 - 2 * way, :, 0:1024], ar.at[axis, way])
            pass_on(axis, 3 - 2 * way)
    for axis in range(2):
        settled(rb.at[axis, 1], sr2.at[axis])
        pass_on(axis, 2)

    def group_rows(g):
        return pl.ds(g * TOK, TOK - CAP if SELF // 4 == g else TOK)

    def halves_from_others(g):
        return sum((o // 4 != 0) + (o % 4 != 0) for o in ORDER[4 * g : 4 * g + 4])

    for n in range(5, 8):
        fetched[n].wait()

    for g in range(4):
        settled(inbox.at[0 : CAP * halves_from_others(g), 0:WIDE], dr.at[g])
        arrived = inbox[g * TOK : (g + 1) * TOK, :]
        gate = nt_dot(arrived, gate_v[...])
        up = nt_dot(arrived, up_v[...])
        hidden = (gate / (1.0 + jnp.exp(-gate)) * up).astype(jnp.bfloat16)
        for h in range(HEADS):
            cols = slice(h * DH, (h + 1) * DH)
            result[g * TOK : (g + 1) * TOK, cols] = jnp.dot(
                hidden, down_v[:, cols], preferred_element_type=jnp.float32
            ).astype(jnp.bfloat16)
        for p in range(pieces):
            for n in range(4 * g, 4 * g + 4):
                if n == SELF:
                    continue
                piece = pl.ds(n * CAP + p * depth, depth)
                back_to = peer_of(me, (4 - ORDER[n] // 4) % 4 * 4 + (4 - ORDER[n] % 4) % 4)
                remote(result.at[piece, :], back.at[piece, :], hs.at[5], br.at[g], back_to).start()
    back[SELF * CAP : (SELF + 1) * CAP, :] = result[SELF * CAP : (SELF + 1) * CAP, :]

    for g in range(4):
        settled(back.at[group_rows(g), :], br.at[g])
        for h in range(HEADS):
            cols = slice(h * DH, (h + 1) * DH)
            both = jnp.dot(wmat[g], back[g * TOK : (g + 1) * TOK, cols], preferred_element_type=jnp.float32)
            total = acc[:, cols] + both[0:TOK, :] + both[TOK : 2 * TOK, :]
            if g < 3:
                acc[:, cols] = total
            else:
                out[:, cols] = total.astype(jnp.bfloat16)

    for n, ref in ((0, gbi), (1, gbf)):
        settled(ref.at[0 : DEV - 1], gs.at[n])
    for n, ref in ((0, kb), (1, vb), (2, qb), (3, ob)):
        settled(ref.at[0 : 7 * TOK, :], hs.at[n])
    settled(mates.at[0:6], gs.at[2])
    settled(disp.at[0 : 12 * CAP, :], hs.at[4])
    settled(result.at[0 : (DEV - 1) * CAP, :], hs.at[5])
    settled(rb, hs.at[6])

    @pl.when(half == 0)
    def _():
        for copy in onward:
            copy.wait_send()


def shards(
    queries, key_vectors, value_vectors, residual_in, input_logit, forget_logit, mix_gain, ffn_gain,
    expert_gate, expert_up, expert_down, routes, route_weight,
):
    hbm = pl.BlockSpec(memory_space=pl.ANY)
    dma = pltpu.SemaphoreType.DMA
    vmem = pltpu.VMEM
    bf16, f32 = jnp.bfloat16, jnp.float32
    return pl.pallas_call(
        kernel,
        out_shape=pltpu.VMEM((TOK, D), bf16),
        in_specs=[hbm] * 13,
        out_specs=pl.BlockSpec(memory_space=pltpu.VMEM),
        scratch_shapes=[
            vmem((8 * TOK, DH), bf16),
            vmem((8 * TOK, DH), bf16),
            vmem((8 * TOK, DH), bf16),
            vmem((4, DH, CHUNK), bf16),
            vmem((DEV, HEADS, TOK), f32),
            vmem((DEV, HEADS, TOK), f32),
            vmem((4, DH, DH), bf16),
            vmem((4, DH, DH), bf16),
            vmem((DH, DH // 2), f32),
            vmem((4, 1, DH), f32),
            vmem((8, DH), f32),
            vmem((2, DH, DH // 2), bf16),
            vmem((2, DH, DH // 2), bf16),
            vmem((8, DH), f32),
            vmem((8 * TOK, DH), bf16),
            vmem((HEADS, TOK, DH), bf16),
            vmem((8, CHUNK), f32),
            vmem((8, CHUNK), f32),
            vmem((4, 1, CHUNK), f32),
            vmem((4, CHUNK, 8), f32),
            vmem((TOK, D), bf16),
            vmem((1, D), f32),
            vmem((1, D), f32),
            vmem((2, TOK), jnp.int32),
            vmem((2, TOK), f32),
            vmem((FF, D), bf16),
            vmem((FF, D), bf16),
            vmem((FF, D), bf16),
            vmem((DEV * CAP, D), bf16),
            vmem((DEV * CAP, D), bf16),
            vmem((DEV * CAP, D), bf16),
            vmem((DEV * CAP, D), bf16),
            vmem((TOK, D), bf16),
            vmem((TOK, D), bf16),
            vmem((2, 4, TOK, TOK), bf16),
            vmem((4, 2 * TOK, TOK), bf16),
            vmem((TOK, D), f32),
            vmem((2, 3, TOK, WIDE), bf16),
            vmem((DEV, 2, TOK), jnp.int32),
            dma((5,)),
            dma((8,)),
            dma((3,)),
            dma((3,)),
            dma((7,)),
            dma((4,)),
            dma((8,)),
            dma((1,)),
            dma((3,)),
            dma((3,)),
            dma((4,)),
            dma((4,)),
            dma((2, 2, 2)),
            dma((2, 2)),
            dma((2,)),
        ],
        compiler_params=pltpu.CompilerParams(
            collective_id=0, has_side_effects=True, vmem_limit_bytes=62 << 20
        ),
        name="block",
    )(
        queries,
        key_vectors,
        value_vectors,
        input_logit,
        forget_logit,
        residual_in,
        mix_gain.reshape(1, D),
        ffn_gain.reshape(1, D),
        jnp.transpose(routes),
        jnp.transpose(route_weight),
        jnp.swapaxes(expert_gate[0], 0, 1),
        jnp.swapaxes(expert_up[0], 0, 1),
        expert_down[0],
    )


def solution(mesh):
    return jax.shard_map(
        shards,
        mesh=mesh,
        in_specs=(
            P(("batch", "seq"), None),
            P(("batch", "seq"), None),
            P(("batch", "seq"), None),
            P(("batch", "seq"), None),
            P(None, ("batch", "seq")),
            P(None, ("batch", "seq")),
            P(),
            P(),
            P("seq", None, None),
            P("seq", None, None),
            P("seq", None, None),
            P(("batch", "seq"), None),
            P(("batch", "seq"), None),
        ),
        out_specs=P(("batch", "seq"), None),
        check_vma=False,
    )
```

```python
import functools
import math

import jax
import jax.numpy as jnp
from jax import lax
from jax.experimental import pallas as pl
from jax.experimental.pallas import tpu as pltpu
from jax.sharding import PartitionSpec as P

NEG_FILL = -1e30
EPSILON = 1e-06
MESH = pl.DeviceIdType.MESH
HEADS = 8
DH = 512
D = 4096
FF = 704
TOK = 128
CAP = 32
DEV = 16
CHUNK = 256
ROOT = 1.0 / math.sqrt(DH)
ORDER = (5, 15, 7, 13, 6, 14, 9, 11, 10, 2, 8, 12, 0, 1, 3, 4)
SELF = ORDER.index(0)
WIDE = D // 2
NEAR = ((0, 1), (0, 3), (1, 0), (1, 1), (1, 3), (0, 2), (1, 2))


def peer_of(me, offset):
    row = lax.rem(me // 4 + offset // 4, 4)
    col = lax.rem(lax.rem(me, 4) + offset % 4, 4)
    return row * 4 + col


def entry_barrier(me):
    barrier = pltpu.get_barrier_semaphore()
    for offset in range(1, DEV):
        pl.semaphore_signal(
            barrier, inc=1, device_id={"seq": peer_of(me, offset)}, device_id_type=MESH
        )
    pl.semaphore_wait(barrier, DEV - 1)


def remote(src, dst, send, recv, device):
    return pltpu.make_async_remote_copy(
        src_ref=src,
        dst_ref=dst,
        send_sem=send,
        recv_sem=recv,
        device_id={"seq": device},
        device_id_type=MESH,
    )


def settled(ref, semaphore):
    pltpu.make_async_copy(ref, ref, semaphore).wait()


def scan_lanes(x, op, fill):
    lane = lax.broadcasted_iota(jnp.int32, x.shape, 1)
    step = 1
    while step < x.shape[1]:
        x = op(x, jnp.where(lane >= step, pltpu.roll(x, step, 1), fill))
        step *= 2
    return x


def three_parts(x):
    high = x.astype(jnp.bfloat16).astype(jnp.float32)
    rest = x - high
    middle = rest.astype(jnp.bfloat16).astype(jnp.float32)
    return high, middle, rest - middle


def nt_dot(a, b):
    return lax.dot_general(a, b, (((1,), (1,)), ((), ())), preferred_element_type=jnp.float32)


def kernel(
    q_in, k_in, v_in, gate_i, gate_f, residual_in, gain_m, gain_f, routes_in, share_in, w_gate, w_up, w_down, out,
    qb, kb, vb, kwt, gbi, gbf, chi, clo, sacc, zst, z_in, st_in, st_out, z_out, ob, mix, rowi, rowf, grow, tcol,
    residual, mix_gain, ffn_gain, routes, route_weight,
    gate_v, up_v, down_v, disp, inbox, result, back, upd, normed, picks, wmat, acc, rb, mates,
    own_sem, w_sem, gs, gr, hs, hr, qr, orr, ss, sr, dr, br, fr, ar, sr2,
):
    me = lax.axis_index("seq")
    half = me // 8
    base = half * 8
    local = me - base
    pair = local // 2
    head = lax.rem(local + 4 * half, 8)

    def rows(j):
        return pl.ds(pl.multiple_of(j * TOK, TOK), TOK)

    def head_columns(h):
        return pl.ds(pl.multiple_of(h * DH, DH), DH)

    own = [
        pltpu.make_async_copy(src.at[:, head_columns(head)], dst, own_sem.at[n])
        for n, (src, dst) in enumerate(
            ((k_in, kb.at[rows(local), :]), (v_in, vb.at[rows(local), :]), (q_in, qb.at[rows(local), :]))
        )
    ]
    own_gates = [
        pltpu.make_async_copy(gate_i, gbi.at[me], own_sem.at[3]),
        pltpu.make_async_copy(gate_f, gbf.at[me], own_sem.at[4]),
    ]
    fetched = [
        pltpu.make_async_copy(src, dst, w_sem.at[n])
        for n, (src, dst) in enumerate(
            (
                (routes_in, routes),
                (share_in, route_weight),
                (gain_m, mix_gain),
                (gain_f, ffn_gain),
                (residual_in, residual),
                (w_gate, gate_v),
                (w_up, up_v),
                (w_down, down_v),
            )
        )
    ]
    for copy in own + own_gates + fetched:
        copy.start()
    entry_barrier(me)

    for offset in range(1, DEV):
        to = peer_of(me, offset)
        for src, dst, n in ((gate_i, gbi, 0), (gate_f, gbf, 1)):
            remote(src, dst.at[me], gs.at[n], gr.at[n], to).start()

    def along(axis, d):
        return peer_of(me, d if axis == 0 else 4 * d)

    for axis in range(2):
        for d in range(1, 4):
            remote(routes_in, mates.at[me], gs.at[2], gr.at[2], along(axis, d)).start()

    def send_part(src, dst, send, recv, lo, width, to):
        to_head = lax.rem(to + 4 * half, 8)
        part = pl.ds(pl.multiple_of(to_head * DH + lo, width), width)
        remote(src.at[:, part], dst.at[rows(local), lo : lo + width], send, recv, base + to).start()

    for src, dst, k in ((k_in, kb, 0), (v_in, vb, 1)):
        for part in range(2):
            for dy, dx in NEAR:
                to = lax.rem(local // 4 + dy, 2) * 4 + lax.rem(lax.rem(local, 4) + dx, 4)
                send_part(src, dst, hs.at[k], hr.at[2 * k + part], part * 256, 256, to)
    for n in range(7):
        if n < 6:
            to = 2 * lax.rem(pair + 3 - n // 2, 4) + n % 2
        else:
            to = 2 * pair + 1 - lax.rem(local, 2)
        send_part(q_in, qb, hs.at[2], qr.at[local], 0, DH, to)

    for n in range(4):
        fetched[n].wait()
    owner = jnp.zeros((DEV, TOK), jnp.int32)
    row16 = lax.broadcasted_iota(jnp.int32, (DEV, TOK), 0)
    for n, offset in enumerate(ORDER):
        owner = jnp.where(row16 == n, peer_of(me, offset), owner)
    hit0 = routes[0:1, :] == owner
    hit1 = routes[1:2, :] == owner
    match = jnp.where(hit0 | hit1, 1.0, 0.0).astype(jnp.bfloat16)
    earlier = lax.broadcasted_iota(jnp.int32, (TOK, TOK), 0) < lax.broadcasted_iota(
        jnp.int32, (TOK, TOK), 1
    )
    position = jnp.dot(
        match, jnp.where(earlier, 1.0, 0.0).astype(jnp.bfloat16), preferred_element_type=jnp.float32
    )
    slot = position + (row16 * CAP).astype(jnp.float32)
    slot0 = jnp.sum(jnp.where(hit0, slot, 0.0), axis=0, keepdims=True)
    slot1 = jnp.sum(jnp.where(hit1, slot, 0.0), axis=0, keepdims=True)
    row8 = lax.broadcasted_iota(jnp.int32, (8, TOK), 0)
    packed = jnp.where(
        row8 == 0,
        slot0,
        jnp.where(row8 == 1, slot1, jnp.where(row8 == 2, route_weight[0:1, :], route_weight[1:2, :])),
    )
    columns = jnp.transpose(packed)
    lane = lax.broadcasted_iota(jnp.int32, (TOK, DEV * CAP), 1).astype(jnp.float32)
    share = jnp.where(lane == columns[:, 0:1], columns[:, 2:3], 0.0) + jnp.where(
        lane == columns[:, 1:2], columns[:, 3:4], 0.0
    )
    high = share.astype(jnp.bfloat16)
    low = (share - high.astype(jnp.float32)).astype(jnp.bfloat16)
    for g in range(4):
        wmat[g, 0:TOK, :] = high[:, g * TOK : (g + 1) * TOK]
        wmat[g, TOK : 2 * TOK, :] = low[:, g * TOK : (g + 1) * TOK]

    settled(mates.at[0:6], gr.at[2])
    target = lax.broadcasted_iota(jnp.int32, (TOK, TOK), 0).astype(jnp.float32)
    upper = jnp.where(earlier, 1.0, 0.0).astype(jnp.bfloat16)
    for axis in range(2):
        owner = jnp.full((DEV, TOK), -1, jnp.int32)
        for t in range(4):
            owner = jnp.where(row16 == t, along(1 - axis, t), owner)
        for d in range(4):
            named = routes[...] if d == 0 else mates[along(axis, d)]
            hit0 = named[0:1, :] == owner
            hit1 = named[1:2, :] == owner
            match = jnp.where(hit0 | hit1, 1.0, 0.0).astype(jnp.bfloat16)
            slot = jnp.dot(match, upper, preferred_element_type=jnp.float32) + (row16 * CAP + 1).astype(jnp.float32)
            slot0 = jnp.sum(jnp.where(hit0, slot, 0.0), axis=0, keepdims=True) - 1.0
            slot1 = jnp.sum(jnp.where(hit1, slot, 0.0), axis=0, keepdims=True) - 1.0
            pick = jnp.where((target == slot0) | (target == slot1), 1.0, 0.0)
            picks[axis, d] = pick.astype(jnp.bfloat16)

    for copy in own_gates:
        copy.wait()
    for n, ref in ((0, gbi), (1, gbf)):
        settled(ref.at[0 : DEV - 1], gr.at[n])
    for b in range(DEV):
        rowi[b // 2 : b // 2 + 1, (b % 2) * TOK : (b % 2 + 1) * TOK] = gbi[b, pl.ds(head, 1), :]
        rowf[b // 2 : b // 2 + 1, (b % 2) * TOK : (b % 2 + 1) * TOK] = gbf[b, pl.ds(head, 1), :]
    x = rowf[...]
    log_forget = jnp.minimum(x, 0.0) - jnp.log1p(jnp.exp(-jnp.abs(x)))
    cumul = scan_lanes(log_forget, jnp.add, 0.0)
    lift = rowi[...] - cumul
    lift_max = scan_lanes(lift, jnp.maximum, NEG_FILL)
    decay = cumul[:, CHUNK - 1 : CHUNK]
    peak_in = decay + lift_max[:, CHUNK - 1 : CHUNK]
    peaks = [jnp.full((1, 1), NEG_FILL, jnp.float32)]
    for c in range(8):
        peaks.append(jnp.maximum(decay[c : c + 1] + peaks[-1], peak_in[c : c + 1]))
    first = half == 0
    scales = []
    since = jnp.ones((1, 1), jnp.float32)
    row8 = lax.broadcasted_iota(jnp.int32, (8, CHUNK), 0)
    for c in range(4):
        before = jnp.where(first, peaks[c], peaks[4 + c])
        after = jnp.where(first, peaks[c + 1], peaks[5 + c])
        dec = jnp.where(first, decay[c : c + 1], decay[4 + c : 5 + c])
        lift_c = jnp.where(first, lift[c : c + 1], lift[4 + c : 5 + c])
        top = jnp.maximum(jnp.where(first, lift_max[c : c + 1], lift_max[4 + c : 5 + c]), before)
        weight = jnp.exp(dec + lift_c - after)
        reach = jnp.exp(before - top) * ROOT
        packed = jnp.where(
            row8 == 0, weight, jnp.where(row8 == 1, top, jnp.where(row8 == 2, reach, reach * since))
        )
        tcol[c] = jnp.transpose(packed)
        grow[c] = lift_c
        scales.append(jnp.exp(dec + before - after))
        since = since * scales[-1]

    z_now = jnp.zeros((1, DH), jnp.float32)
    own[0].wait()
    own[1].wait()
    for part in range(2):
        settled(kb.at[0 : 7 * TOK, part * 256 : part * 256 + 256], hr.at[part])
    for c in range(4):
        weighted = kb[c * CHUNK : (c + 1) * CHUNK, :].astype(jnp.float32) * tcol[c][:, 0:1]
        kwt[c] = jnp.transpose(weighted.astype(jnp.bfloat16))
        zst[c] = z_now
        z_now = scales[c] * z_now + jnp.sum(weighted, axis=0, keepdims=True)
    z_out[...] = jnp.broadcast_to(z_now, (8, DH))
    chi[0] = jnp.zeros((DH, DH), jnp.bfloat16)
    clo[0] = jnp.zeros((DH, DH), jnp.bfloat16)

    next_device = 8 + lax.rem(local + 4, 8)
    onward = [remote(z_out, z_in, ss.at[2], sr.at[2], next_device)] + [
        remote(st_out.at[part], st_in.at[part], ss.at[part], sr.at[part], next_device) for part in range(2)
    ]
    for part in range(2):
        cols = slice(part * 256, part * 256 + 256)
        settled(vb.at[0 : 7 * TOK, cols], hr.at[2 + part])
        for c in range(4):
            state = jnp.dot(kwt[c], vb[c * CHUNK : (c + 1) * CHUNK, cols], preferred_element_type=jnp.float32)
            if c > 0:
                state += scales[c] * sacc[...]
            high = state.astype(jnp.bfloat16)
            if c < 3:
                sacc[...] = state
                chi[c + 1, :, cols] = high
                clo[c + 1, :, cols] = (state - high.astype(jnp.float32)).astype(jnp.bfloat16)
            else:
                st_out[part] = high

        @pl.when(half == 0)
        def _():
            if part == 0:
                onward[0].start()
            onward[1 + part].start()

    @pl.when(half == 0)
    def _():
        z_in[...] = jnp.zeros((8, DH), jnp.float32)

    @pl.when(half == 1)
    def _():
        for copy in onward:
            copy.wait_recv()

    causal = lax.broadcasted_iota(jnp.int32, (CHUNK, CHUNK), 0) >= lax.broadcasted_iota(
        jnp.int32, (CHUNK, CHUNK), 1
    )
    z_row = lax.broadcasted_iota(jnp.int32, (8, DH), 0)

    @pl.loop(0, 4)
    def _(i):
        c = lax.rem(i + 1 + pair, 4)
        for jj in range(2):
            j = 2 * c + jj

            @pl.when(j != local)
            def _():
                settled(qb.at[rows(j), :], qr.at[j])

            @pl.when(j == local)
            def _():
                own[2].wait()

        part = pl.ds(pl.multiple_of(c * CHUNK, CHUNK), CHUNK)
        query = qb[part, :]
        value = vb[part, :]
        columns = tcol[c]
        top, reach, reach0 = columns[:, 1:2], columns[:, 2:3], columns[:, 3:4]
        weight = jnp.exp(jnp.where(causal, grow[c] - top, NEG_FILL))
        coef = weight * (nt_dot(query, kb[part, :]) * ROOT)
        denom = jnp.sum(coef, axis=1, keepdims=True)
        numer = jnp.dot(coef.astype(jnp.bfloat16), value, preferred_element_type=jnp.float32)
        held = jnp.dot(query, chi[c], preferred_element_type=jnp.float32)
        held += jnp.dot(query, clo[c], preferred_element_type=jnp.float32)
        parts = three_parts(zst[c]) + three_parts(z_in[0:1, :])
        z_all = jnp.zeros((8, DH), jnp.float32)
        for n, piece in enumerate(parts):
            z_all = jnp.where(z_row == n, piece, z_all)
        norm = nt_dot(query, z_all.astype(jnp.bfloat16))
        denom += reach * (norm[:, 0:1] + norm[:, 1:2] + norm[:, 2:3])
        denom += reach0 * (norm[:, 3:4] + norm[:, 4:5] + norm[:, 5:6])
        numer += reach * held

        def finish(total):
            ob[part, :] = (total / jnp.maximum(jnp.abs(denom), 1.0)).astype(jnp.bfloat16)

        @pl.when(half == 0)
        def _():
            finish(numer)

        @pl.when(half == 1)
        def _():
            from_first = jnp.concatenate(
                [jnp.dot(query, st_in[n], preferred_element_type=jnp.float32) for n in range(2)], axis=1
            )
            finish(numer + reach0 * from_first)

        for jj in range(2):
            j = 2 * c + jj

            @pl.when(j != local)
            def _():
                remote(ob.at[rows(j), :], mix.at[head], hs.at[3], orr.at[0], base + j).start()

            @pl.when(j == local)
            def _():
                mix[head] = ob[rows(j), :]

    fetched[4].wait()
    settled(mix.at[0:7], orr.at[0])
    square = jnp.zeros((TOK, 1), jnp.float32)
    for h in range(HEADS):
        part = mix[h].astype(jnp.float32)
        square += jnp.sum(part * part, axis=1, keepdims=True)
    scale = lax.rsqrt(square * (1.0 / D) + EPSILON)
    square = jnp.zeros((TOK, 1), jnp.float32)
    for h in range(HEADS):
        cols = slice(h * DH, (h + 1) * DH)
        part = residual[:, cols].astype(jnp.float32) + mix[h].astype(jnp.float32) * scale * mix_gain[:, cols]
        rounded = part.astype(jnp.bfloat16)
        upd[:, cols] = rounded
        part = rounded.astype(jnp.float32)
        square += jnp.sum(part * part, axis=1, keepdims=True)
    scale = lax.rsqrt(square * (1.0 / D) + EPSILON)
    for h in range(HEADS):
        cols = slice(h * DH, (h + 1) * DH)
        part = upd[:, cols].astype(jnp.float32)
        acc[:, cols] = part
        normed[:, cols] = (part * scale * ffn_gain[:, cols]).astype(jnp.bfloat16)

    def quarter(p):
        return slice(p * 512, p * 512 + 512)

    def gather_sems(axis, way, p):
        if p // 2 == way:
            return fr.at[axis, way, p % 2]
        return ar.at[axis, way]

    for k in range(4):
        for axis in range(2):
            for way in range(2):
                p = (k + 2 * way) % 4
                remote(
                    normed.at[:, axis * WIDE + p * 512 : axis * WIDE + p * 512 + 512],
                    rb.at[axis, 2 - 2 * way, :, quarter(p)],
                    hs.at[6],
                    gather_sems(axis, way, p),
                    along(axis, 1 + 2 * way),
                ).start()

    def block_of(axis, d, t):
        back_d = (4 - d) % 4
        return ORDER.index(t * 4 + back_d if axis == 0 else back_d * 4 + t)

    def pass_on(axis, d):
        for p in range(4):
            cols = slice(axis * WIDE + p * 512, axis * WIDE + p * 512 + 512)
            rows_here = normed[:, cols] if d == 0 else rb[axis, d - 1, :, quarter(p)]
            picked = jnp.dot(picks[axis, d], rows_here, preferred_element_type=jnp.float32)
            disp[d * TOK : (d + 1) * TOK, cols] = picked.astype(jnp.bfloat16)
        cols = slice(axis * WIDE, (axis + 1) * WIDE)
        for part in range(2):
            for t in (1, 3, 2):
                n = block_of(axis, d, t)
                remote(
                    disp.at[pl.ds(d * TOK + t * CAP + part * 16, 16), cols],
                    inbox.at[pl.ds(n * CAP + part * 16, 16), cols],
                    hs.at[4],
                    dr.at[n // 4],
                    along(1 - axis, t),
                ).start()
        n = block_of(axis, d, 0)
        inbox[n * CAP : (n + 1) * CAP, cols] = disp[d * TOK : d * TOK + CAP, cols]

    pass_on(0, 0)
    pass_on(1, 0)
    for k in range(2):
        for axis in range(2):
            for way in range(2):
                p = 2 * way + k
                came = rb.at[axis, 2 - 2 * way, :, quarter(p)]
                settled(came, fr.at[axis, way, k])
                remote(came, rb.at[axis, 1, :, quarter(p)], hs.at[6], sr2.at[axis], along(axis, 1 + 2 * way)).start()
    for axis in range(2):
        for way in range(2):
            settled(rb.at[axis, 2 - 2 * way, :, 0:1024], ar.at[axis, way])
            pass_on(axis, 3 - 2 * way)
    for axis in range(2):
        settled(rb.at[axis, 1], sr2.at[axis])
        pass_on(axis, 2)

    def group_rows(g):
        return pl.ds(g * TOK, TOK - CAP if SELF // 4 == g else TOK)

    def halves_from_others(g):
        return sum((o // 4 != 0) + (o % 4 != 0) for o in ORDER[4 * g : 4 * g + 4])

    for n in range(5, 8):
        fetched[n].wait()

    for g in range(4):
        settled(inbox.at[0 : CAP * halves_from_others(g), 0:WIDE], dr.at[g])
        arrived = inbox[g * TOK : (g + 1) * TOK, :]
        gate = nt_dot(arrived, gate_v[...])
        up = nt_dot(arrived, up_v[...])
        hidden = (gate / (1.0 + jnp.exp(-gate)) * up).astype(jnp.bfloat16)
        for side in range(2):
            for h in range(4 * side, 4 * side + 4):
                cols = slice(h * DH, (h + 1) * DH)
                result[g * TOK : (g + 1) * TOK, cols] = jnp.dot(
                    hidden, down_v[:, cols], preferred_element_type=jnp.float32
                ).astype(jnp.bfloat16)
            cols = slice(side * WIDE, (side + 1) * WIDE)
            for part in range(2):
                for n in range(4 * g, 4 * g + 4):
                    if n == SELF:
                        continue
                    piece = pl.ds(n * CAP + part * 16, 16)
                    back_to = peer_of(me, (4 - ORDER[n] // 4) % 4 * 4 + (4 - ORDER[n] % 4) % 4)
                    remote(result.at[piece, cols], back.at[piece, cols], hs.at[5], br.at[g], back_to).start()
    back[SELF * CAP : (SELF + 1) * CAP, :] = result[SELF * CAP : (SELF + 1) * CAP, :]

    for turn, g in enumerate(range(4)):
        settled(back.at[group_rows(g), :], br.at[g])
        for h in range(HEADS):
            cols = slice(h * DH, (h + 1) * DH)
            both = jnp.dot(wmat[g], back[g * TOK : (g + 1) * TOK, cols], preferred_element_type=jnp.float32)
            total = acc[:, cols] + both[0:TOK, :] + both[TOK : 2 * TOK, :]
            if turn < 3:
                acc[:, cols] = total
            else:
                out[:, cols] = total.astype(jnp.bfloat16)

    for n, ref in ((0, gbi), (1, gbf)):
        settled(ref.at[0 : DEV - 1], gs.at[n])
    for n, ref in ((0, kb), (1, vb), (2, qb), (3, ob)):
        settled(ref.at[0 : 7 * TOK, :], hs.at[n])
    settled(mates.at[0:6], gs.at[2])
    settled(disp.at[0 : 12 * CAP, :], hs.at[4])
    settled(result.at[0 : (DEV - 1) * CAP, :], hs.at[5])
    settled(rb, hs.at[6])

    @pl.when(half == 0)
    def _():
        for copy in onward:
            copy.wait_send()


def shards(
    queries, key_vectors, value_vectors, residual_in, input_logit, forget_logit, mix_gain, ffn_gain,
    expert_gate, expert_up, expert_down, routes, route_weight,
):
    hbm = pl.BlockSpec(memory_space=pl.ANY)
    dma = pltpu.SemaphoreType.DMA
    vmem = pltpu.VMEM
    bf16, f32 = jnp.bfloat16, jnp.float32
    return pl.pallas_call(
        kernel,
        out_shape=pltpu.VMEM((TOK, D), bf16),
        in_specs=[hbm] * 13,
        out_specs=pl.BlockSpec(memory_space=pltpu.VMEM),
        scratch_shapes=[
            vmem((8 * TOK, DH), bf16),
            vmem((8 * TOK, DH), bf16),
            vmem((8 * TOK, DH), bf16),
            vmem((4, DH, CHUNK), bf16),
            vmem((DEV, HEADS, TOK), f32),
            vmem((DEV, HEADS, TOK), f32),
            vmem((4, DH, DH), bf16),
            vmem((4, DH, DH), bf16),
            vmem((DH, DH // 2), f32),
            vmem((4, 1, DH), f32),
            vmem((8, DH), f32),
            vmem((2, DH, DH // 2), bf16),
            vmem((2, DH, DH // 2), bf16),
            vmem((8, DH), f32),
            vmem((8 * TOK, DH), bf16),
            vmem((HEADS, TOK, DH), bf16),
            vmem((8, CHUNK), f32),
            vmem((8, CHUNK), f32),
            vmem((4, 1, CHUNK), f32),
            vmem((4, CHUNK, 8), f32),
            vmem((TOK, D), bf16),
            vmem((1, D), f32),
            vmem((1, D), f32),
            vmem((2, TOK), jnp.int32),
            vmem((2, TOK), f32),
            vmem((FF, D), bf16),
            vmem((FF, D), bf16),
            vmem((FF, D), bf16),
            vmem((DEV * CAP, D), bf16),
            vmem((DEV * CAP, D), bf16),
            vmem((DEV * CAP, D), bf16),
            vmem((DEV * CAP, D), bf16),
            vmem((TOK, D), bf16),
            vmem((TOK, D), bf16),
            vmem((2, 4, TOK, TOK), bf16),
            vmem((4, 2 * TOK, TOK), bf16),
            vmem((TOK, D), f32),
            vmem((2, 3, TOK, WIDE), bf16),
            vmem((DEV, 2, TOK), jnp.int32),
            dma((5,)),
            dma((8,)),
            dma((3,)),
            dma((3,)),
            dma((7,)),
            dma((4,)),
            dma((8,)),
            dma((1,)),
            dma((3,)),
            dma((3,)),
            dma((4,)),
            dma((4,)),
            dma((2, 2, 2)),
            dma((2, 2)),
            dma((2,)),
        ],
        compiler_params=pltpu.CompilerParams(
            collective_id=0, has_side_effects=True, vmem_limit_bytes=62 << 20
        ),
        name="block",
    )(
        queries,
        key_vectors,
        value_vectors,
        input_logit,
        forget_logit,
        residual_in,
        mix_gain.reshape(1, D),
        ffn_gain.reshape(1, D),
        jnp.transpose(routes),
        jnp.transpose(route_weight),
        jnp.swapaxes(expert_gate[0], 0, 1),
        jnp.swapaxes(expert_up[0], 0, 1),
        expert_down[0],
    )


def solution(mesh):
    return jax.shard_map(
        shards,
        mesh=mesh,
        in_specs=(
            P(("batch", "seq"), None),
            P(("batch", "seq"), None),
            P(("batch", "seq"), None),
            P(("batch", "seq"), None),
            P(None, ("batch", "seq")),
            P(None, ("batch", "seq")),
            P(),
            P(),
            P("seq", None, None),
            P("seq", None, None),
            P("seq", None, None),
            P(("batch", "seq"), None),
            P(("batch", "seq"), None),
        ),
        out_specs=P(("batch", "seq"), None),
        check_vma=False,
    )
```
